32 devices in a mesh: leaf: 8 (over z, y), grid: 4 (over x, core).
Axes of the slice: x: 2, y: 2, z: 4, core: 2. Of those that a mesh axis runs over, the one named last changes fastest.
Arguments:
- source_leaf: float32 [8, 4096], P(None, ('leaf', 'grid')), may hold values from -6 to 6
- block_leaf: float32 [4096, 128], P(('leaf', 'grid')), may hold values from -0.5 to 0.5
- expand_leaf: float32 [4096, 128], P(('leaf', 'grid')), may hold values from -0.5 to 0.5
- basis_leaf: float32 [4096, 256], P(('leaf', 'grid')), may hold values from -0.25 to 0.25
- pivot_leaf: float32 [4096], P(('leaf', 'grid')), may hold values from -2 to 2
- couple_leaf: float32 [8192, 128], P(('leaf', 'grid')), may hold values from -0.5 to 0.5
- ranks_leaf: int32 [8, 2], replicated, may hold values from 32 to 128
- targets_leaf: int32 [8192], P(('leaf', 'grid')), may hold values from 0 to 2047, as said below
- source_middle: float32 [8, 4096], P(None, ('leaf', 'grid')), may hold values from -6 to 6
- block_middle: float32 [4096, 128], P(('leaf', 'grid')), may hold values from -0.5 to 0.5
- expand_middle: float32 [4096, 128], P(('leaf', 'grid')), may hold values from -0.5 to 0.5
- basis_middle: float32 [4096, 256], P(('leaf', 'grid')), may hold values from -0.1875 to 0.1875
- pivot_middle: float32 [4096], P(('leaf', 'grid')), may hold values from -2 to 2
- couple_middle: float32 [4096, 128], P(('leaf', 'grid')), may hold values from -0.5 to 0.5
- ranks_middle: int32 [4, 2], replicated, may hold values from 32 to 128
- targets_middle: int32 [4096], P(('leaf', 'grid')), may hold values from 0 to 4095, as said below
- source_upper: float32 [8, 4096], P(None, ('leaf', 'grid')), may hold values from -6 to 6
- block_upper: float32 [4096, 128], P(('leaf', 'grid')), may hold values from -0.5 to 0.5
- expand_upper: float32 [4096, 128], P(('leaf', 'grid')), may hold values from -0.5 to 0.5
- basis_upper: float32 [4096, 256], P(('leaf', 'grid')), may hold values from -0.125 to 0.125
- pivot_upper: float32 [4096], P(('leaf', 'grid')), may hold values from -2 to 2
- couple_upper: float32 [4096, 128], P(('leaf', 'grid')), may hold values from -0.5 to 0.5
- ranks_upper: int32 [2, 2], replicated, may hold values from 32 to 128
- targets_upper: int32 [4096], P(('leaf', 'grid')), may hold values from 0 to 4095, as said below
- source_root: float32 [8, 4096], P(None, ('leaf', 'grid')), may hold values from -6 to 6
- block_root: float32 [4096, 128], P(('leaf', 'grid')), may hold values from -0.5 to 0.5
- expand_root: float32 [4096, 128], P(('leaf', 'grid')), may hold values from -0.5 to 0.5
- basis_root: float32 [4096, 256], P(('leaf', 'grid')), may hold values from -0.09375 to 0.09375
- pivot_root: float32 [4096], P(('leaf', 'grid')), may hold values from -2 to 2
- ranks_root: int32 [1, 2], replicated, may hold values from 32 to 128
Outputs:
- answer_leaf: float32 [8, 4096], P(None, ('leaf', 'grid'))
- answer_middle: float32 [8, 4096], P(None, ('leaf', 'grid'))
- answer_upper: float32 [8, 4096], P(None, ('leaf', 'grid'))
- answer_root: float32 [8, 4096], P(None, ('leaf', 'grid'))
The draws below stay inside these ranges and needn't reach their ends.
Inputs may be any that keep to these rules, and one draw needn't show every extreme that they name: `targets_leaf`: within one leaf front the 1024 entries are distinct; each names a row of the parent front's row vector of 2048 rows. Split that vector's separator part and its update part each evenly, in order, over the parent's devices (leaf then grid); then the rows of one device name at most 32 rows held by any one of them, and exactly that many for some. `targets_middle`: within one middle front the entries are distinct; each names a row of the parent front's row vector of 4096 rows. Split likewise over the parent's devices, the rows of one device name at most 8 rows held by any one of them, and exactly that many for some. `targets_upper`: within one upper front the entries are distinct; each names a row of the root separator. Split evenly in order over all devices, the rows of one device name at most 4 rows held by any one of them, and exactly that many for some.
All inputs are finite; a program needn't handle non-finite values.
Results may differ from the reference program's by a relative error of at most 0.0003.
Values sent between devices are 32-bit elements; how exact they have to be, the bound alone decides.
A program may use at most 128 MiB of HBM per device.

```python
import jax
import jax.numpy as jnp
from jax import lax

RHS_COUNT = 8
BLOCK = 128
RANK = 128
TOP_ROWS = 128
SEP_LEAF = 512
UPD_LEAF = 1024
SEP_MID = 1024
SEP_UP = 2048
SEP_ROOT = 4096
N_LEAF = 8
N_GRID = 4


def pick_rows(key, salt, fronts, count, owners, width, pieces, sep_rows):
    base = jax.random.fold_in(key, salt)
    slots_each = pieces * width

    def one_front(front):
        fkey = jax.random.fold_in(base, front)
        order = jax.random.permutation(jax.random.fold_in(fkey, 1), owners)
        slot_keys = jax.vmap(lambda owner: jax.random.fold_in(jax.random.fold_in(fkey, 2), owner))(jnp.arange(owners, dtype=jnp.int32))
        slot_order = jax.vmap(lambda one: jax.random.permutation(one, slots_each))(slot_keys)
        rows = jnp.arange(count, dtype=jnp.int32)
        owner = order[rows % owners]
        slot = slot_order[owner, rows // owners]
        return slot // width * sep_rows + owner * width + slot % width
    picked = jax.vmap(one_front)(jnp.arange(fronts, dtype=jnp.int32))
    return picked.reshape(-1).astype(jnp.int32)


def draw_targets_leaf(key, part):
    return pick_rows(key, 11, N_LEAF, UPD_LEAF, N_LEAF * N_GRID // 4, TOP_ROWS, 2, SEP_MID)


def draw_targets_middle(key, part):
    return pick_rows(key, 12, 4, SEP_MID, N_LEAF * N_GRID // 2, TOP_ROWS, 2, SEP_UP)


def draw_targets_upper(key, part):
    return pick_rows(key, 13, 2, SEP_UP, N_LEAF * N_GRID, TOP_ROWS, 1, SEP_ROOT)


def set_ends(array, own_key, low, top_value):
    longest = array.shape.index(max(array.shape))
    spots = []
    for shift in (0, 1):
        where = [jax.random.randint(jax.random.fold_in(own_key, axis), (), 0, length) for axis, length in enumerate(array.shape)]
        where[longest] = (where[longest] + shift) % array.shape[longest]
        spots.append(tuple(where))
    return array.at[spots[0]].set(low).at[spots[1]].set(top_value)


def level_of(rng, dims, shards, least, high):
    def one(position, blocks):
        heights = jax.random.uniform(jax.random.fold_in(jax.random.fold_in(rng, 6), position), (blocks,), jnp.float32, least / len(shards), high / len(shards))
        return jnp.repeat(jnp.exp(heights), dims[position] // blocks).reshape((-1,) + (1,) * (len(dims) - position - 1))

    factor_of = one(*shards[0])
    for cut in shards[1:]:
        factor_of = factor_of * one(*cut)
    return factor_of


def centred(key, dims, scale, limit, shards=(), held_as=jnp.bfloat16):
    factor_of = level_of(key, dims, shards, -0.22, 0.18) if shards else 1.0
    values = jax.random.normal(key, dims, jnp.float32) * scale * factor_of
    return jnp.minimum(jnp.maximum(values, -limit), limit).astype(held_as)


def setup_inputs(seed: int = 0) -> dict:
    key_list = jax.random.split(jax.random.key(seed), 31)
    return {
        "source_leaf": centred(key_list[0], (RHS_COUNT, N_LEAF * SEP_LEAF), 1.0, 6.0, ((1, 32),), jnp.float32),
        "block_leaf": centred(key_list[1], (N_LEAF * SEP_LEAF, BLOCK), BLOCK ** -0.5, 0.5, ((0, 32),), jnp.float32),
        "expand_leaf": centred(key_list[2], (N_LEAF * SEP_LEAF, RANK), RANK ** -0.5, 0.5, ((0, 32),), jnp.float32),
        "basis_leaf": centred(key_list[3], (N_LEAF * SEP_LEAF, 2 * RANK), SEP_LEAF ** -0.5, 0.25, ((0, 32),), jnp.float32),
        "pivot_leaf": jnp.clip(jax.random.uniform(key_list[4], (N_LEAF * SEP_LEAF,), jnp.float32, -2.0, 2.0) * level_of(key_list[4], (N_LEAF * SEP_LEAF,), ((0, 32),), -0.4, 0.0), -2.0, 2.0),
        "couple_leaf": centred(key_list[5], (N_LEAF * UPD_LEAF, RANK), RANK ** -0.5, 0.5, ((0, 32),), jnp.float32),
        "ranks_leaf": set_ends(jax.random.randint(key_list[6], (N_LEAF, 2), RANK // 4, RANK + 1), jax.random.fold_in(key_list[6], 1), RANK // 4, RANK).astype(jnp.int32),
        "targets_leaf": draw_targets_leaf(jax.random.fold_in(key_list[30], 71), 0),
        "source_middle": centred(key_list[8], (RHS_COUNT, 4 * SEP_MID), 1.0, 6.0, ((1, 32),), jnp.float32),
        "block_middle": centred(key_list[9], (4 * SEP_MID, BLOCK), BLOCK ** -0.5, 0.5, ((0, 32),), jnp.float32),
        "expand_middle": centred(key_list[10], (4 * SEP_MID, RANK), RANK ** -0.5, 0.5, ((0, 32),), jnp.float32),
        "basis_middle": centred(key_list[11], (4 * SEP_MID, 2 * RANK), SEP_MID ** -0.5, 0.1875, ((0, 32),), jnp.float32),
        "pivot_middle": jnp.clip(jax.random.uniform(key_list[12], (4 * SEP_MID,), jnp.float32, -2.0, 2.0) * level_of(key_list[12], (4 * SEP_MID,), ((0, 32),), -0.4, 0.0), -2.0, 2.0),
        "couple_middle": centred(key_list[13], (4 * SEP_MID, RANK), RANK ** -0.5, 0.5, ((0, 32),), jnp.float32),
        "ranks_middle": set_ends(jax.random.randint(key_list[14], (4, 2), RANK // 4, RANK + 1), jax.random.fold_in(key_list[14], 1), RANK // 4, RANK).astype(jnp.int32),
        "targets_middle": draw_targets_middle(jax.random.fold_in(key_list[30], 71), 0),
        "source_upper": centred(key_list[16], (RHS_COUNT, 2 * SEP_UP), 1.0, 6.0, ((1, 32),), jnp.float32),
        "block_upper": centred(key_list[17], (2 * SEP_UP, BLOCK), BLOCK ** -0.5, 0.5, ((0, 32),), jnp.float32),
        "expand_upper": centred(key_list[18], (2 * SEP_UP, RANK), RANK ** -0.5, 0.5, ((0, 32),), jnp.float32),
        "basis_upper": centred(key_list[19], (2 * SEP_UP, 2 * RANK), SEP_UP ** -0.5, 0.125, ((0, 32),), jnp.float32),
        "pivot_upper": jnp.clip(jax.random.uniform(key_list[20], (2 * SEP_UP,), jnp.float32, -2.0, 2.0) * level_of(key_list[20], (2 * SEP_UP,), ((0, 32),), -0.4, 0.0), -2.0, 2.0),
        "couple_upper": centred(key_list[21], (2 * SEP_UP, RANK), RANK ** -0.5, 0.5, ((0, 32),), jnp.float32),
        "ranks_upper": set_ends(jax.random.randint(key_list[22], (2, 2), RANK // 4, RANK + 1), jax.random.fold_in(key_list[22], 1), RANK // 4, RANK).astype(jnp.int32),
        "targets_upper": draw_targets_upper(jax.random.fold_in(key_list[30], 71), 0),
        "source_root": centred(key_list[24], (RHS_COUNT, SEP_ROOT), 1.0, 6.0, ((1, 32),), jnp.float32),
        "block_root": centred(key_list[25], (SEP_ROOT, BLOCK), BLOCK ** -0.5, 0.5, ((0, 32),), jnp.float32),
        "expand_root": centred(key_list[26], (SEP_ROOT, RANK), RANK ** -0.5, 0.5, ((0, 32),), jnp.float32),
        "basis_root": centred(key_list[27], (SEP_ROOT, 2 * RANK), SEP_ROOT ** -0.5, 0.09375, ((0, 32),), jnp.float32),
        "pivot_root": jnp.clip(jax.random.uniform(key_list[28], (SEP_ROOT,), jnp.float32, -2.0, 2.0) * level_of(key_list[28], (SEP_ROOT,), ((0, 32),), -0.4, 0.0), -2.0, 2.0),
        "ranks_root": jax.random.randint(key_list[29], (1, 2), RANK // 4, RANK + 1).astype(jnp.int32),
    }


HIGH_PRECISION = lax.Precision.HIGHEST


def make_masks(ranks):
    cols = jnp.arange(RANK, dtype=jnp.int32)
    head_mask_grid = (cols[None, :] < ranks[:, 0:1]).astype(jnp.float32)[:, None, :]
    column_mask_grid = (cols[None, :] < ranks[:, 1:2]).astype(jnp.float32)[:, None, :]
    return head_mask_grid, column_mask_grid


def forward(source, inc_sep, block, expand, basis, pivot, ranks, fronts):
    width = source.shape[1] // fronts
    level_batch_index = source.reshape(RHS_COUNT, fronts, width).transpose(1, 0, 2)
    if inc_sep is not None:
        level_batch_index = level_batch_index + inc_sep
    tiles = block.reshape(fronts, width // BLOCK, BLOCK, BLOCK)
    local_portion = jnp.einsum("fanh,fnhk->fank", level_batch_index.reshape(fronts, RHS_COUNT, width // BLOCK, BLOCK), tiles, precision=HIGH_PRECISION).reshape(fronts, RHS_COUNT, width)
    gens = basis.reshape(fronts, width, 2 * RANK)
    query_lookup = gens[:, :, :RANK]
    coupling_right_factor = gens[:, :, RANK:]
    spread_across_rows = expand.reshape(fronts, width, RANK)
    head_mask_grid, column_mask_grid = make_masks(ranks)
    hidden_query_rows = jnp.einsum("mle,meq->mlq", level_batch_index, query_lookup, precision=HIGH_PRECISION) * head_mask_grid
    intermediate_entries = local_portion + jnp.einsum("gdk,gtk->gdt", hidden_query_rows, spread_across_rows, precision=HIGH_PRECISION)
    weight_entries = jnp.einsum("mle,meq->mlq", intermediate_entries, coupling_right_factor, precision=HIGH_PRECISION) * column_mask_grid
    correction_entries = intermediate_entries * pivot.reshape(fronts, 1, width)
    return correction_entries, weight_entries, (tiles, query_lookup, coupling_right_factor, spread_across_rows, head_mask_grid, column_mask_grid)


def flat_index(targets, fronts, parents, total):
    count = targets.shape[0] // fronts
    owner = jnp.arange(fronts, dtype=jnp.int32) // (fronts // parents)
    return (owner[:, None] * total + targets.reshape(fronts, count).astype(jnp.int32)).reshape(-1)


def scatter_up(update, targets, fronts, parents, sep_par, upd_par):
    total = sep_par + upd_par
    flat = flat_index(targets, fronts, parents, total)
    values = update.transpose(1, 0, 2).reshape(RHS_COUNT, -1)
    buffer = jnp.zeros((RHS_COUNT, parents * total), jnp.float32).at[:, flat].add(values)
    buffer = buffer.reshape(RHS_COUNT, parents, total).transpose(1, 0, 2)
    return buffer[:, :, :sep_par], buffer[:, :, sep_par:]


def pull_down(front_rows, targets, fronts, parents):
    total = front_rows.shape[2]
    flat = flat_index(targets, fronts, parents, total)
    whole = front_rows.transpose(1, 0, 2).reshape(RHS_COUNT, parents * total)
    values = jnp.take(whole, flat, axis=1)
    return values.reshape(RHS_COUNT, fronts, -1).transpose(1, 0, 2)


def backward(correction_entries, x_upd, couple, parts, fronts):
    tiles, query_lookup, coupling_right_factor, spread_across_rows, head_mask_grid, column_mask_grid = parts
    width = correction_entries.shape[2]
    remainder_rows = correction_entries
    if x_upd is not None:
        couple_u = couple.reshape(fronts, -1, RANK)
        solve_direction = jnp.einsum("fau,fur->far", x_upd, couple_u, precision=HIGH_PRECISION) * column_mask_grid
        remainder_rows = correction_entries - jnp.einsum("gdk,gtk->gdt", solve_direction, coupling_right_factor, precision=HIGH_PRECISION)
    right_projection = jnp.einsum("mle,meq->mlq", remainder_rows, spread_across_rows, precision=HIGH_PRECISION) * head_mask_grid
    local_portion = jnp.einsum("fanh,fnkh->fank", remainder_rows.reshape(fronts, RHS_COUNT, width // BLOCK, BLOCK), tiles, precision=HIGH_PRECISION).reshape(fronts, RHS_COUNT, width)
    return local_portion + jnp.einsum("gdk,gtk->gdt", right_projection, query_lookup, precision=HIGH_PRECISION)


def reference(source_leaf, block_leaf, expand_leaf, basis_leaf, pivot_leaf, couple_leaf, ranks_leaf, targets_leaf,
              source_middle, block_middle, expand_middle, basis_middle, pivot_middle, couple_middle, ranks_middle, targets_middle,
              source_upper, block_upper, expand_upper, basis_upper, pivot_upper, couple_upper, ranks_upper, targets_upper,
              source_root, block_root, expand_root, basis_root, pivot_root, ranks_root):
    levels = [
        (source_leaf, block_leaf, expand_leaf, basis_leaf, pivot_leaf, couple_leaf, ranks_leaf, targets_leaf),
        (source_middle, block_middle, expand_middle, basis_middle, pivot_middle, couple_middle, ranks_middle, targets_middle),
        (source_upper, block_upper, expand_upper, basis_upper, pivot_upper, couple_upper, ranks_upper, targets_upper),
        (source_root, block_root, expand_root, basis_root, pivot_root, None, ranks_root, None),
    ]
    fronts = [N_LEAF, 4, 2, 1]
    inc_sep = None
    inc_upd = None
    saved = []
    for level in range(4):
        source, block, expand, basis, pivot, couple, ranks, targets = levels[level]
        correction_entries, weight_entries, parts = forward(source, inc_sep, block, expand, basis, pivot, ranks, fronts[level])
        saved.append((correction_entries, parts))
        if level < 3:
            couple_u = couple.reshape(fronts[level], -1, RANK)
            update = -jnp.einsum("far,fur->fau", weight_entries, couple_u, precision=HIGH_PRECISION)
            if inc_upd is not None:
                update = update + inc_upd
            sep_par = levels[level + 1][0].shape[1] // fronts[level + 1]
            upd_par = 0
            if level + 1 < 3:
                upd_par = levels[level + 1][5].shape[0] // fronts[level + 1]
            inc_sep, inc_upd = scatter_up(update, targets, fronts[level], fronts[level + 1], sep_par, upd_par)
            if upd_par == 0:
                inc_upd = None
    answers = [None, None, None, None]
    rows_par = None
    for level in (3, 2, 1, 0):
        correction_entries, parts = saved[level]
        couple = levels[level][5]
        targets = levels[level][7]
        x_upd = None
        if level < 3:
            x_upd = pull_down(rows_par, targets, fronts[level], fronts[level + 1])
        xvals = backward(correction_entries, x_upd, couple, parts, fronts[level])
        answers[level] = xvals.transpose(1, 0, 2).reshape(RHS_COUNT, -1)
        rows_par = xvals if x_upd is None else jnp.concatenate([xvals, x_upd], axis=2)
    return (answers[0], answers[1], answers[2], answers[3])
```

```python
import functools

import jax
import jax.numpy as jnp
from jax import lax
from jax.experimental import pallas as pl
from jax.experimental.pallas import tpu as pltpu
from jax.sharding import PartitionSpec as P

RANK = 128
LANES = 128
MESH = pl.DeviceIdType.MESH
HIGHEST = lax.Precision.HIGHEST
F32 = jnp.float32
BF16 = jnp.bfloat16


def dot(a, b, ca, cb, precision=HIGHEST):
    return lax.dot_general(
        a, b, (((ca,), (cb,)), ((), ())), precision=precision, preferred_element_type=F32
    )


def mult(a, b):
    return dot(a, b, 1, 0)


def outer(a, b):
    return dot(a, b, 1, 1)


def inner(a, b):
    return dot(a, b, 0, 0)


def split3(x):
    hi = x.astype(BF16).astype(F32)
    rest = x - hi
    mid = rest.astype(BF16).astype(F32)
    return jnp.concatenate([hi, mid, rest - mid], axis=0).astype(BF16)


def select(x, onehot, cb):
    out = dot(split3(x), onehot, 1, cb, lax.Precision.DEFAULT)
    n = x.shape[0]
    return out[:n] + out[n : 2 * n] + out[2 * n :]


def kernel(cfg, *refs):
    leaves, across, size, ups, count = cfg
    total_devices = leaves * across
    (src, blk, exp, bas, piv, rnk) = [refs[4 * i : 4 * i + 4] for i in range(6)]
    cpl = refs[24:27]
    tgt = refs[27:30]
    outs = refs[30:34]
    (f1, f2, f3, f4, f5, b1, b2, b3) = refs[34:42]
    fwd = (f1, f2, f3)
    bwd = (b3, b2, b1)
    perm_buf = refs[42:45]
    recv_c = refs[45:48]
    cross_p = refs[48:51]
    rs_buf = refs[51:54]
    cross_all = refs[54:57]
    tg_buf = (None,) + tuple(refs[57:59])
    bot = (None,) + tuple(refs[59:61])
    fts = refs[61:-5]
    ft = (None, fts[0], fts[-1])
    gt = refs[-5:-2]
    send_sem, recv_sem = refs[-2:]

    me = lax.axis_index("leaf") * across + lax.axis_index("grid")
    pending = []

    def where(peer):
        return (peer // across, peer % across)

    def remote(a, b, sem, peer):
        return pltpu.make_async_remote_copy(
            src_ref=a,
            dst_ref=b,
            send_sem=send_sem.at[sem],
            recv_sem=recv_sem.at[sem],
            device_id=where(peer),
            device_id_type=MESH,
        )

    def wait_for(part, sem):
        pltpu.make_async_copy(part, part, sem).wait()

    def send_all(buf, group, sem):
        idx = me % group
        base = me - idx

        def body(k, carry):
            peer = base + (idx + k) % group
            remote(buf.at[idx], buf.at[idx], sem, peer).start()
            return carry

        lax.fori_loop(1, group, body, 0)
        pending.append((buf.at[pl.ds(0, group - 1)], sem))

    def arrive(buf, group, sem):
        wait_for(buf.at[pl.ds(0, group - 1)], recv_sem.at[sem])

    barrier = pltpu.get_barrier_semaphore()

    def greet(k, carry):
        pl.semaphore_signal(
            barrier, inc=1, device_id=where((me + k) % total_devices), device_id_type=MESH
        )
        return carry

    lax.fori_loop(1, total_devices, greet, 0)

    col = lax.broadcasted_iota(jnp.int32, (count, RANK), 1)

    def mask(level, front, which):
        return (col < rnk[level][front, which]).astype(F32)

    def local_forward(level, b):
        local = mult(b, blk[level][...])
        bq = mult(b, bas[level][:, :RANK])
        lv = mult(local, bas[level][:, RANK:]) if level < 3 else None
        return local, bq, lv

    b = src[0][...]
    local, bq, lv = local_forward(0, b)
    idx = me % size[1]
    f1[idx] = jnp.concatenate([bq, lv], axis=0)
    for level in range(3):
        cross_p[level][...] = inner(exp[level][...], bas[level][:, RANK:])
    pl.semaphore_wait(barrier, total_devices - 1)
    send_all(f1, size[1], 0)

    parts_of = [min(size[level], 16) for level in range(3)]
    for level in range(3):
        g = size[level]
        p = parts_of[level]
        rp = RANK // p
        idx = me % g
        base = me - idx
        sem = 8 + level
        start = 1 if g == p else 0

        def scatter(k, carry, level=level, g=g, p=p, rp=rp, idx=idx, base=base, sem=sem):
            q = (idx + k) % p

            def go():
                rows = pl.ds(pl.multiple_of(q * rp, 8), rp)
                remote(cross_p[level].at[rows], rs_buf[level].at[idx], sem, base + q).start()

            if g == p:
                go()
            else:
                pl.when(q != idx)(go)
            return carry

        lax.fori_loop(start, p, scatter, 0)

        def keep(level=level, rp=rp, idx=idx):
            rows = pl.ds(pl.multiple_of(idx * rp, 8), rp)
            rs_buf[level][idx] = cross_p[level][rows, :]

        if g == p:
            keep()
        else:
            pl.when(idx < p)(keep)

    for level in (1, 2):
        gp = size[level + 1]
        tg_buf[level][me % gp] = jnp.broadcast_to(tgt[level][...], (8, LANES)).astype(F32)
        send_all(tg_buf[level], gp, 14 + level)

    for level in range(3):
        gp = size[level + 1]
        u = ups[level]
        cap = perm_buf[level].shape[1]
        sep = gp * LANES
        t = tgt[level][...]
        upd = t >= sep
        rel = jnp.where(upd, t - sep, t)
        dst = rel // LANES
        low = rel % LANES + jnp.where(upd, LANES, 0)
        ri = lax.broadcasted_iota(jnp.int32, (u, u), 0)
        ci = lax.broadcasted_iota(jnp.int32, (u, u), 1)
        dst_f = dst.astype(F32)
        dst_c = jnp.sum(jnp.where(ri == ci, jnp.broadcast_to(dst_f, (u, u)), 0.0), axis=1, keepdims=True)
        rank = jnp.sum(
            jnp.where((dst_c == dst_f) & (ri < ci), 1.0, 0.0), axis=0, keepdims=True
        ).astype(jnp.int32)
        pos = dst * cap + rank
        slots = gp * cap
        si = lax.broadcasted_iota(jnp.int32, (slots, u), 0)
        hit = (si == pos).astype(F32)
        moved = mult(hit, cpl[level][...])
        lowc = jnp.sum(hit * low.astype(F32), axis=1, keepdims=True)
        both = jnp.concatenate([moved, jnp.broadcast_to(lowc, (slots, LANES))], axis=1)
        perm_buf[level][...] = both.reshape(gp, cap, 2 * LANES)
        idx = me % gp
        base = me - idx
        recv_c[level][idx] = perm_buf[level][idx]

        def ship(k, carry, level=level, gp=gp, idx=idx, base=base):
            q = (idx + k) % gp
            remote(perm_buf[level].at[q], recv_c[level].at[idx], 11 + level, base + q).start()
            return carry

        lax.fori_loop(1, gp, ship, 0)
        pending.append((perm_buf[level].at[pl.ds(0, gp - 1)], 11 + level))

    for level in range(3):
        g = size[level]
        gp = size[level + 1]
        p = parts_of[level]
        rp = RANK // p
        nch = gp // g
        idx = me % g
        place = me % gp
        base = me - place
        sem = 17 + level
        slot = place // g * p + idx

        def gather(level=level, g=g, gp=gp, idx=idx, place=place, base=base, sem=sem, slot=slot):
            wait_for(rs_buf[level].at[pl.ds(0, g - 1)], recv_sem.at[8 + level])
            cross_all[level][slot] = jnp.sum(rs_buf[level][...], axis=0)

            def body(k, carry):
                peer = base + (place + k) % gp
                part = cross_all[level].at[slot]
                remote(part, part, sem, peer).start()
                return carry

            lax.fori_loop(1, gp, body, 0)

        if g == p:
            gather()
        else:
            pl.when(idx < p)(gather)

    late = total_devices > 64

    def build_ft(level):
        chunk = LANES
        t = tgt[level][...]
        ri = lax.broadcasted_iota(jnp.int32, (chunk, LANES), 0)

        def fill_ft(j, carry):
            rows = pl.ds(pl.multiple_of(j * chunk, chunk), chunk)
            ft[level][rows, :] = (ri + j * chunk == t).astype(F32).astype(BF16)
            return carry

        lax.fori_loop(0, ft[level].shape[0] // chunk, fill_ft, 0)

    for level in (1, 2):
        gp = size[level + 1]
        place = me % gp
        rows = bot[level].shape[0]
        ri = lax.broadcasted_iota(jnp.int32, (rows, LANES), 0)
        arrive(tg_buf[level], gp, 14 + level)
        mine = jnp.where(ri < LANES, place * LANES + ri, (gp + place - 1) * LANES + ri).astype(F32)

        def fill(j, carry, level=level, mine=mine):
            t = tg_buf[level][j][0:1, :]
            lanes = pl.ds(pl.multiple_of(j * LANES, LANES), LANES)
            bot[level][:, lanes] = (mine == t).astype(F32).astype(BF16)
            return carry

        lax.fori_loop(0, gp, fill, 0)
        if not late:
            build_ft(level)

    def build_gt(level):
        g = size[level]
        gp = size[level + 1]
        cap = recv_c[level].shape[1]
        nch = gp // g
        rows = gt[level].shape[1]
        arrive(recv_c[level], gp, 11 + level)
        slots = g * cap
        lane = lax.broadcasted_iota(jnp.int32, (slots, rows), 1).astype(F32)
        for child in range(nch):
            got = recv_c[level][child * g : (child + 1) * g].reshape(slots, 2 * LANES)
            ot = (lane == got[:, LANES : LANES + 1]).astype(F32)
            gt[level][child * RANK : (child + 1) * RANK, :] = inner(got[:, :LANES], ot)

    def arrive_cross(level):
        g = size[level]
        p = parts_of[level]
        n = size[level + 1] // g * p
        sem = 17 + level
        if g == p:
            wait_for(cross_all[level].at[pl.ds(0, n - 1)], recv_sem.at[sem])
        else:
            idx = me % g
            pl.when(idx < p)(lambda: wait_for(cross_all[level].at[pl.ds(0, n - 1)], recv_sem.at[sem]))
            pl.when(idx >= p)(lambda: wait_for(cross_all[level].at[pl.ds(0, n)], recv_sem.at[sem]))

    def cross_of(level, child):
        p = parts_of[level]
        return cross_all[level][pl.ds(child * p, p)].reshape(RANK, RANK)

    saved = []
    z_total = []
    inc_upd = None
    for level in range(3):
        g = size[level]
        gp = size[level + 1]
        nch = gp // g
        place = me % gp
        parent = me // gp
        child_me = place // g
        build_gt(level)
        arrive_cross(level)
        buf = fwd[level]
        arrive(buf, gp, level)
        ws = []
        for child in range(nch):
            tot = jnp.sum(buf[child * g : (child + 1) * g, : 2 * count, :], axis=0)
            front = parent * nch + child
            hq = tot[:count] * mask(level, front, 0)
            cross = cross_of(level, child)
            ws.append((tot[count:] + mult(hq, cross)) * mask(level, front, 1))
        inc = -mult(jnp.concatenate(ws, axis=1), gt[level][...])
        if inc_upd is not None:
            rows = jnp.concatenate([buf[j, 2 * count : 3 * count, :] for j in range(gp)], axis=1)
            inc = inc + select(rows, bot[level][...], 1)
            below = size[level - 1]
            first = place // below * below
            z_total.append(jnp.sum(buf[pl.ds(first, below), 3 * count : 4 * count, :], axis=0))
        bn = src[level + 1][...] + inc[:, :LANES]
        local_n, bq_n, lv_n = local_forward(level + 1, bn)
        own = jnp.sum(buf[pl.ds(child_me * g, g), :count, :], axis=0)
        hq = own * mask(level, me // g, 0)
        y = local + outer(hq, exp[level][...])
        z = y * piv[level][...]
        saved.append(z)
        zp = mult(z, exp[level][...])
        if level < 2:
            inc_upd = inc[:, LANES:]
            nxt = fwd[level + 1]
            gn = size[level + 2]
            nxt[me % gn] = jnp.concatenate([bq_n, lv_n, inc_upd, zp], axis=0)
            send_all(nxt, gn, level + 1)
        else:
            f4[me % gp] = jnp.concatenate([bq_n, zp], axis=0)
            send_all(f4, gp, 3)
        local = local_n

    top = size[3]
    place = me % top
    arrive(f4, top, 3)
    tot = jnp.sum(f4[:, :count, :], axis=0)
    below = size[2]
    z_total.append(jnp.sum(f4[pl.ds(place // below * below, below), count:, :], axis=0))
    hq = tot * mask(3, 0, 0)
    z = (local + outer(hq, exp[3][...])) * piv[3][...]
    f5[place] = mult(z, exp[3][...])
    send_all(f5, top, 4)
    base_x = outer(z, blk[3][...])
    arrive(f5, top, 4)
    rp_total = jnp.sum(f5[...], axis=0) * mask(3, 0, 0)
    x = base_x + outer(rp_total, bas[3][:, :RANK])
    outs[3][...] = x

    xu = None
    for level in (2, 1, 0):
        g = size[level]
        gp = size[level + 1]
        nch = gp // g
        place = me % gp
        child_me = place // g
        buf = bwd[level]
        full = x if xu is None else jnp.concatenate([x, xu], axis=1)
        sp = outer(full, gt[level][...])
        pieces = [sp[:, c * RANK : (c + 1) * RANK] for c in range(nch)]
        if level > 0:
            pieces = pieces + ([x] if xu is None else [x, xu])
        buf[place] = jnp.concatenate(pieces, axis=0)
        send_all(buf, gp, 5 + (2 - level))
        arrive(buf, gp, 5 + (2 - level))
        rows = pl.ds(pl.multiple_of(child_me * count, count), count)
        s = jnp.sum(buf[:, rows, :], axis=0) * mask(level, me // g, 1)
        if level > 0:
            o = nch * count
            blocks = [buf[j, o : o + count, :] for j in range(gp)]
            if xu is not None:
                blocks += [buf[j, o + count : o + 2 * count, :] for j in range(gp)]
            if late:
                build_ft(level)
            xu = select(jnp.concatenate(blocks, axis=1), ft[level][...], 0)
        r = saved[level] - outer(s, bas[level][:, RANK:])
        proj = (z_total[level] - outer(s, cross_of(level, child_me))) * mask(level, me // g, 0)
        x = outer(r, blk[level][...]) + outer(proj, bas[level][:, :RANK])
        outs[level][...] = x

    for part, sem in pending:
        wait_for(part, send_sem.at[sem])
    for level in range(3):
        g = size[level]
        gp = size[level + 1]
        p = parts_of[level]
        rp = RANK // p
        n = gp // g * p
        idx = me % g

        def rs_done(pieces, level=level, rp=rp):
            wait_for(cross_p[level].at[pl.ds(0, pieces * rp)], send_sem.at[8 + level])

        def ag_done(level=level, g=g, p=p, n=n):
            for _ in range(g // p - 1):
                wait_for(cross_all[level].at[pl.ds(0, n)], send_sem.at[17 + level])
            wait_for(cross_all[level].at[pl.ds(0, n - 1)], send_sem.at[17 + level])

        if g == p:
            rs_done(p - 1)
            ag_done()
        else:
            pl.when(idx < p)(functools.partial(rs_done, p - 1))
            pl.when(idx >= p)(functools.partial(rs_done, p))
            pl.when(idx < p)(ag_done)


def solution(mesh):
    leaves, across = mesh.shape["leaf"], mesh.shape["grid"]

    def shards(*args):
        levels = [args[8 * i : 8 * i + 8] for i in range(3)]
        root = args[24:30]
        (sl, bl, el, qs, pv, cl, rk, tg) = zip(*levels)
        src = list(sl) + [root[0]]
        blk = list(bl) + [root[1]]
        exp = list(el) + [root[2]]
        bas = list(qs) + [root[3]]
        piv = [v.reshape(1, -1) for v in list(pv) + [root[4]]]
        rnk = list(rk) + [root[5]]
        tgt = [t.reshape(1, -1) for t in tg]
        count = src[0].shape[0]
        ups = [t.shape[1] for t in tgt]
        fronts = [r.shape[0] for r in rnk]
        size = [leaves * across // f for f in fronts]
        for v in src:
            assert v.shape[1] == LANES
        vm = lambda *s: pltpu.VMEM(s, F32)
        nch = [size[i + 1] // size[i] for i in range(3)]
        cap = [max(8, -(-ups[i] // size[i + 1])) for i in range(3)]
        rows = [2 * LANES, 2 * LANES, LANES]
        parts = [min(size[i], 16) for i in range(3)]
        scratch = [
            vm(size[1], 2 * count, LANES),
            vm(size[2], 4 * count, LANES),
            vm(size[3], 4 * count, LANES),
            vm(size[3], 2 * count, LANES),
            vm(size[3], count, LANES),
            vm(size[3], (nch[2] + 1) * count, LANES),
            vm(size[2], (nch[1] + 2) * count, LANES),
            vm(size[1], nch[0] * count, LANES),
        ]
        scratch += [vm(size[i + 1], cap[i], 2 * LANES) for i in range(3)] * 2
        scratch += [vm(RANK, RANK) for i in range(3)]
        scratch += [vm(size[i], RANK // parts[i], RANK) for i in range(3)]
        scratch += [vm(nch[i] * parts[i], RANK // parts[i], RANK) for i in range(3)]
        scratch += [vm(size[i + 1], 8, LANES) for i in (1, 2)]
        scratch += [pltpu.VMEM((rows[i], size[i + 1] * LANES), BF16) for i in (1, 2)]
        fts = (1, 2) if leaves * across <= 64 else (1,)
        scratch += [pltpu.VMEM((size[i + 1] * rows[i], LANES), BF16) for i in fts]
        scratch += [vm(nch[i] * RANK, rows[i]) for i in range(3)]
        scratch += [pltpu.SemaphoreType.DMA((20,)), pltpu.SemaphoreType.DMA((20,))]
        vspec = pl.BlockSpec(memory_space=pltpu.VMEM)
        sspec = pl.BlockSpec(memory_space=pltpu.SMEM)
        return pl.pallas_call(
            functools.partial(kernel, (leaves, across, size, ups, count)),
            out_shape=[jax.ShapeDtypeStruct(v.shape, F32) for v in src],
            in_specs=[vspec] * 20 + [sspec] * 4 + [vspec] * 6,
            out_specs=[vspec] * 4,
            scratch_shapes=scratch,
            compiler_params=pltpu.CompilerParams(
                collective_id=0, has_side_effects=True, vmem_limit_bytes=60 * 1024 * 1024
            ),
        )(*src, *blk, *exp, *bas, *piv, *rnk, *cl, *tgt)

    spread = ("leaf", "grid")
    level = (P(None, spread), P(spread, None), P(spread, None), P(spread, None), P(spread))
    mid = level + (P(spread, None), P(), P(spread))
    return jax.shard_map(
        shards,
        mesh=mesh,
        in_specs=mid * 3 + level + (P(),),
        out_specs=(P(None, spread),) * 4,
        check_vma=False,
    )
```

```python
import functools

import jax
import jax.numpy as jnp
from jax import lax
from jax.experimental import pallas as pl
from jax.experimental.pallas import tpu as pltpu
from jax.sharding import PartitionSpec as P

RANK = 128
LANES = 128
MESH = pl.DeviceIdType.MESH
HIGHEST = lax.Precision.HIGHEST
F32 = jnp.float32
BF16 = jnp.bfloat16


def dot(a, b, ca, cb, precision=HIGHEST):
    return lax.dot_general(
        a, b, (((ca,), (cb,)), ((), ())), precision=precision, preferred_element_type=F32
    )


def mult(a, b):
    return dot(a, b, 1, 0)


def outer(a, b):
    return dot(a, b, 1, 1)


def inner(a, b):
    return dot(a, b, 0, 0)


def split3(x):
    hi = x.astype(BF16).astype(F32)
    rest = x - hi
    mid = rest.astype(BF16).astype(F32)
    return jnp.concatenate([hi, mid, rest - mid], axis=0).astype(BF16)


def select(x, onehot, cb):
    out = dot(split3(x), onehot, 1, cb, lax.Precision.DEFAULT)
    n = x.shape[0]
    return out[:n] + out[n : 2 * n] + out[2 * n :]


def kernel(cfg, names, *refs):
    leaves, across, size, ups, count, caps = cfg
    total_devices = leaves * across
    (src, blk, exp, bas, piv, rnk) = [refs[4 * i : 4 * i + 4] for i in range(6)]
    cpl = refs[24:27]
    tgt = refs[27:30]
    outs = refs[30:34]
    m = dict(zip(names, refs[34:-2]))
    send_sem, recv_sem = refs[-2:]
    sems = {}

    me = lax.axis_index("leaf") * across + lax.axis_index("grid")
    plane = size[1]
    planes = total_devices // plane
    spot = me % plane
    layer = me // plane
    late = total_devices > 64
    pending = []

    def where(peer):
        return (peer // across, peer % across)

    def sem_of(name):
        return sems.setdefault(name, len(sems))

    def remote(a, b, sem, peer):
        return pltpu.make_async_remote_copy(
            src_ref=a,
            dst_ref=b,
            send_sem=send_sem.at[sem],
            recv_sem=recv_sem.at[sem],
            device_id=where(peer),
            device_id_type=MESH,
        )

    def wait_for(part, sem):
        pltpu.make_async_copy(part, part, sem).wait()

    def send_each(source, dest, group, name, stride=1):
        idx = me // stride % group
        base = me - idx * stride
        sem = sem_of(name)

        def body(k, carry):
            q = (idx + k) % group
            remote(source(q), dest(idx), sem, base + q * stride).start()
            return carry

        lax.fori_loop(1, group, body, 0)

    def send_all(name, group, stride=1):
        buf = m[name]
        idx = me // stride % group
        send_each(lambda q: buf.at[idx], lambda i: buf.at[i], group, name, stride)
        pending.append((buf.at[pl.ds(0, group - 1)], sem_of(name)))

    def arrive(name, group):
        wait_for(m[name].at[pl.ds(0, group - 1)], recv_sem.at[sem_of(name)])

    barrier = pltpu.get_barrier_semaphore()

    def greet(k, carry):
        pl.semaphore_signal(
            barrier, inc=1, device_id=where((me + k) % total_devices), device_id_type=MESH
        )
        return carry

    lax.fori_loop(1, total_devices, greet, 0)

    col = lax.broadcasted_iota(jnp.int32, (count, RANK), 1)

    def mask(level, front, which):
        return (col < rnk[level][front, which]).astype(F32)

    def local_forward(level, b):
        local = mult(b, blk[level][...])
        bq = mult(b, bas[level][:, :RANK])
        lv = mult(local, bas[level][:, RANK:]) if level < 3 else None
        return local, bq, lv

    parts_of = [min(size[level], 16) for level in range(3)]

    def scatter_cross(level):
        g = size[level]
        p = parts_of[level]
        rp = RANK // p
        idx = me % g
        base = me - idx
        sem = sem_of(("rs", level))
        cross_p, rs_buf = m["cross_p", level], m["rs", level]

        def body(k, carry):
            q = (idx + k) % p

            def go():
                rows = pl.ds(pl.multiple_of(q * rp, 8), rp)
                remote(cross_p.at[rows], rs_buf.at[idx], sem, base + q).start()

            if g == p:
                go()
            else:
                pl.when(q != idx)(go)
            return carry

        lax.fori_loop(1 if g == p else 0, p, body, 0)

        def keep():
            rows = pl.ds(pl.multiple_of(idx * rp, 8), rp)
            rs_buf[idx] = cross_p[rows, :]

        if g == p:
            keep()
        else:
            pl.when(idx < p)(keep)

    def ship_couple(level):
        gp = size[level + 1]
        u = ups[level]
        cap = caps[level]
        wide = max(8, cap)
        sep = gp * LANES
        t = tgt[level][...]
        upd = t >= sep
        rel = jnp.where(upd, t - sep, t)
        dst = rel // LANES
        low = rel % LANES + jnp.where(upd, LANES, 0)
        ri = lax.broadcasted_iota(jnp.int32, (u, u), 0)
        ci = lax.broadcasted_iota(jnp.int32, (u, u), 1)
        dst_f = dst.astype(F32)
        dst_c = jnp.sum(jnp.where(ri == ci, jnp.broadcast_to(dst_f, (u, u)), 0.0), axis=1, keepdims=True)
        rank = jnp.sum(
            jnp.where((dst_c == dst_f) & (ri < ci), 1.0, 0.0), axis=0, keepdims=True
        ).astype(jnp.int32)
        pos = dst * wide + rank
        slots = gp * wide
        si = lax.broadcasted_iota(jnp.int32, (slots, u), 0)
        hit = (si == pos).astype(F32)
        moved = mult(hit, cpl[level][...])
        perm_buf, recv_c = m["perm", level], m["couple", level]
        if cap <= 4:
            shifted = (si == pos + 4).astype(F32)
            lowc = jnp.sum(shifted * low.astype(F32), axis=1, keepdims=True)
            both = moved + jnp.broadcast_to(lowc, (slots, LANES))
        else:
            lowc = jnp.sum(hit * low.astype(F32), axis=1, keepdims=True)
            both = jnp.concatenate([moved, jnp.broadcast_to(lowc, (slots, LANES))], axis=1)
        perm_buf[...] = both.reshape(gp, wide, both.shape[1])
        idx = me % gp
        recv_c[idx] = perm_buf[idx]
        send_each(lambda q: perm_buf.at[q], lambda i: recv_c.at[i], gp, ("couple", level))
        pending.append((perm_buf.at[pl.ds(0, gp - 1)], sem_of(("couple", level))))

    def gather_cross(level):
        g = size[level]
        gp = size[level + 1]
        p = parts_of[level]
        idx = me % g
        place = me % gp
        sem = sem_of(("cross", level))
        slot = place // g * p + idx
        buf, rs_buf = m["cross", level], m["rs", level]

        def go():
            wait_for(rs_buf.at[pl.ds(0, g - 1)], recv_sem.at[sem_of(("rs", level))])
            buf[slot] = jnp.sum(rs_buf[...], axis=0)

            def body(k, carry):
                peer = me - place + (place + k) % gp
                remote(buf.at[slot], buf.at[slot], sem, peer).start()
                return carry

            lax.fori_loop(1, gp, body, 0)

        if g == p:
            go()
        else:
            pl.when(idx < p)(go)

    def build_gt(level):
        g = size[level]
        gp = size[level + 1]
        wide = max(8, caps[level])
        nch = gp // g
        gt = m["gt", level]
        rows = gt.shape[1]
        arrive(("couple", level), gp)
        slots = g * wide
        lane = lax.broadcasted_iota(jnp.int32, (slots, rows), 1).astype(F32)
        for child in range(nch):
            got = m["couple", level][child * g : (child + 1) * g]
            got = got.reshape(slots, got.shape[2])
            if caps[level] <= 4:
                up = jnp.concatenate([got[4:, :1], got[:4, :1]], axis=0)
                si = lax.broadcasted_iota(jnp.int32, (slots, 1), 0)
                low = jnp.where(si % 8 < 4, up, -1.0)
            else:
                low = got[:, LANES : LANES + 1]
            ot = (lane == low).astype(F32)
            gt[child * RANK : (child + 1) * RANK, :] = inner(got[:, :LANES], ot)

    def arrive_cross(level):
        g = size[level]
        p = parts_of[level]
        n = size[level + 1] // g * p
        sem = recv_sem.at[sem_of(("cross", level))]
        buf = m["cross", level]
        if g == p:
            wait_for(buf.at[pl.ds(0, n - 1)], sem)
        else:
            idx = me % g
            pl.when(idx < p)(lambda: wait_for(buf.at[pl.ds(0, n - 1)], sem))
            pl.when(idx >= p)(lambda: wait_for(buf.at[pl.ds(0, n)], sem))

    def cross_of(level, child):
        p = parts_of[level]
        return m["cross", level][pl.ds(child * p, p)].reshape(RANK, RANK)

    def build_bot_middle():
        gp = size[2]
        place = me % gp
        rows = 2 * LANES
        ri = lax.broadcasted_iota(jnp.int32, (rows, LANES), 0)
        arrive("tgt_middle", gp)
        mine = jnp.where(ri < LANES, place * LANES + ri, (gp + place - 1) * LANES + ri).astype(F32)

        def fill(j, carry):
            t = m["tgt_middle"][j][0:1, :]
            lanes = pl.ds(pl.multiple_of(j * LANES, LANES), LANES)
            m["bot_middle"][:, lanes] = (mine == t).astype(F32).astype(BF16)
            return carry

        lax.fori_loop(0, gp, fill, 0)

    def build_bot_upper():
        rows = planes * LANES
        ri = lax.broadcasted_iota(jnp.int32, (rows, LANES), 0)
        arrive("tgt_upper", plane)
        mine = ((ri // LANES * plane + spot) * LANES + ri % LANES).astype(F32)

        def fill(j, carry):
            t = m["tgt_upper"][j][0:1, :]
            lanes = pl.ds(pl.multiple_of(j * LANES, LANES), LANES)
            m["bot_upper"][:, lanes] = (mine == t).astype(F32).astype(BF16)
            return carry

        lax.fori_loop(0, plane, fill, 0)

    def build_ft_middle():
        t = tgt[1][...]
        ri = lax.broadcasted_iota(jnp.int32, (LANES, LANES), 0)

        def fill(j, carry):
            rows = pl.ds(pl.multiple_of(j * LANES, LANES), LANES)
            m["ft_middle"][rows, :] = (ri + j * LANES == t).astype(F32).astype(BF16)
            return carry

        lax.fori_loop(0, m["ft_middle"].shape[0] // LANES, fill, 0)

    def build_ft_upper():
        arrive("tgt_layer", planes)
        t = jnp.concatenate([m["tgt_layer"][j][0:1, :] for j in range(planes)], axis=1)
        ri = lax.broadcasted_iota(jnp.int32, (LANES, planes * LANES), 0)

        def fill(j, carry):
            rows = pl.ds(pl.multiple_of(j * LANES, LANES), LANES)
            here = ((ri + (layer * plane + j) * LANES).astype(F32) == t).astype(F32)
            m["ft_upper"][rows, :] = here.astype(BF16)
            return carry

        lax.fori_loop(0, plane, fill, 0)

    def total_sum(value, name):
        m[name, "a"][spot] = value
        send_all((name, "a"), plane)
        arrive((name, "a"), plane)
        m[name, "b"][layer] = jnp.sum(m[name, "a"][...], axis=0)
        send_all((name, "b"), planes, plane)

    def total_arrived(name):
        arrive((name, "b"), planes)
        return jnp.sum(m[name, "b"][...], axis=0)

    def share(level, zp):
        m["zp", level][me % size[level]] = zp
        send_all(("zp", level), size[level])

    def shared(level):
        arrive(("zp", level), size[level])
        return jnp.sum(m["zp", level][...], axis=0)

    local, bq, lv = local_forward(0, src[0][...])
    m["f1"][spot] = jnp.concatenate([bq, lv], axis=0)
    m["cross_p", 0][...] = inner(exp[0][...], bas[0][:, RANK:])
    pl.semaphore_wait(barrier, total_devices - 1)
    send_all("f1", plane)
    scatter_cross(0)
    ship_couple(0)
    for level in (1, 2):
        m["cross_p", level][...] = inner(exp[level][...], bas[level][:, RANK:])
        scatter_cross(level)
    m["tgt_middle"][me % size[2]] = jnp.broadcast_to(tgt[1][...], (8, LANES)).astype(F32)
    send_all("tgt_middle", size[2])
    gather_cross(0)
    ship_couple(1)
    gather_cross(1)
    mine_t = jnp.broadcast_to(tgt[2][...], (8, LANES)).astype(F32)
    m["tgt_upper"][spot] = mine_t
    send_all("tgt_upper", plane)
    m["tgt_layer"][layer] = mine_t
    send_all("tgt_layer", planes, plane)
    build_gt(0)

    saved = []
    inc_upd = None
    for level in range(3):
        g = size[level]
        gp = size[level + 1]
        nch = gp // g
        place = me % gp
        parent = me // gp
        child_me = place // g
        arrive_cross(level)
        if level < 2:
            name = ("f1", "f2")[level]
            buf, step = m[name], g
            arrive(name, gp)
        else:
            buf, step = m["f3b"], g // plane
            arrive("f3b", planes)
        ws = []
        for child in range(nch):
            tot = jnp.sum(buf[child * step : (child + 1) * step, : 2 * count, :], axis=0)
            front = parent * nch + child
            hq = tot[:count] * mask(level, front, 0)
            cross = cross_of(level, child)
            ws.append((tot[count:] + mult(hq, cross)) * mask(level, front, 1))
        inc = -mult(jnp.concatenate(ws, axis=1), m["gt", level][...])
        if level == 1:
            rows = jnp.concatenate([buf[j, 2 * count : 3 * count, :] for j in range(gp)], axis=1)
            inc = inc + select(rows, m["bot_middle"][...], 1)
        if level == 2:
            inc = inc + jnp.sum(buf[:, 2 * count : 3 * count, :], axis=0)
        bn = src[level + 1][...] + inc[:, :LANES]
        local_n, bq_n, lv_n = local_forward(level + 1, bn)
        if level == 0:
            m["f2"][me % size[2]] = jnp.concatenate([bq_n, lv_n, inc[:, LANES:]], axis=0)
            send_all("f2", size[2])
        elif level == 1:
            m["f3a"][spot] = jnp.concatenate([bq_n, lv_n, inc[:, LANES:]], axis=0)
            send_all("f3a", plane)
        else:
            m["f4", "a"][spot] = bq_n
            send_all(("f4", "a"), plane)
        own = jnp.sum(buf[pl.ds(child_me * step, step), :count, :], axis=0)
        hq = own * mask(level, me // g, 0)
        z = (local + outer(hq, exp[level][...])) * piv[level][...]
        saved.append(z)
        share(level, mult(z, exp[level][...]))
        if level == 0:
            ship_couple(2)
            gather_cross(2)
            build_gt(1)
            build_bot_middle()
        elif level == 1:
            build_bot_upper()
            arrive("f3a", plane)
            sums = jnp.sum(m["f3a"][:, : 2 * count, :], axis=0)
            rows = jnp.concatenate([m["f3a"][j, 2 * count :, :] for j in range(plane)], axis=1)
            part = select(rows, m["bot_upper"][...], 1)
            for q in range(planes):
                m["f3s"][q] = jnp.concatenate([sums, part[:, q * LANES : (q + 1) * LANES]], axis=0)
            m["f3b"][layer] = m["f3s"][layer]
            send_each(lambda q: m["f3s"].at[q], lambda i: m["f3b"].at[i], planes, "f3b", plane)
            pending.append((m["f3s"].at[pl.ds(0, planes - 1)], sem_of("f3b")))
            build_gt(2)
        else:
            arrive(("f4", "a"), plane)
            m["f4", "b"][layer] = jnp.sum(m["f4", "a"][...], axis=0)
            send_all(("f4", "b"), planes, plane)
        local = local_n

    build_ft_upper()
    hq = total_arrived("f4") * mask(3, 0, 0)
    z = (local + outer(hq, exp[3][...])) * piv[3][...]
    total_sum(mult(z, exp[3][...]), "f5")
    if not late:
        build_ft_middle()
    x = outer(z, blk[3][...])
    rp_total = total_arrived("f5") * mask(3, 0, 0)
    x = x + outer(rp_total, bas[3][:, :RANK])

    xu = None
    for level in (2, 1, 0):
        g = size[level]
        gp = size[level + 1]
        nch = gp // g
        place = me % gp
        child_me = place // g
        full = x if xu is None else jnp.concatenate([x, xu], axis=1)
        sp = outer(full, m["gt", level][...])
        pieces = [sp[:, c * RANK : (c + 1) * RANK] for c in range(nch)]
        if level == 2:
            m["b1a"][spot] = jnp.concatenate(pieces + [x], axis=0)
            send_all("b1a", plane)
            outs[3][...] = x
            arrive("b1a", plane)
            o = nch * count
            sums = jnp.sum(m["b1a"][:, :o, :], axis=0)
            rows = jnp.concatenate([m["b1a"][j, o:, :] for j in range(plane)], axis=1)
            part = select(rows, m["ft_upper"][...], 0)
            for q in range(planes):
                c = q * plane // g
                m["b1s"][q] = jnp.concatenate(
                    [sums[c * count : (c + 1) * count], part[:, q * LANES : (q + 1) * LANES]], axis=0
                )
            m["b1b"][layer] = m["b1s"][layer]
            send_each(lambda q: m["b1s"].at[q], lambda i: m["b1b"].at[i], planes, "b1b", plane)
            pending.append((m["b1s"].at[pl.ds(0, planes - 1)], sem_of("b1b")))
            arrive("b1b", planes)
            both = jnp.sum(m["b1b"][...], axis=0)
            s, xu = both[:count], both[count:]
        else:
            name = ("b3", "b2")[level]
            buf, piece = m[name], m["piece", level]
            for c in range(nch):
                piece[c] = pieces[c]
            head = pl.ds(0, count)
            rest = pl.ds(count, 2 * count)
            buf[place, head] = piece[child_me]
            if level == 1:
                buf[place, rest] = jnp.concatenate([x, xu], axis=0)

                def ship(k, carry, gp=gp, g=g, place=place, buf=buf, piece=piece, name=name):
                    q = (place + k) % gp
                    peer = me - place + q
                    sem = sem_of(name)
                    remote(piece.at[q // g], buf.at[place, head], sem, peer).start()
                    remote(buf.at[place, rest], buf.at[place, rest], sem, peer).start()
                    return carry

                lax.fori_loop(1, gp, ship, 0)
            else:
                send_each(lambda q: piece.at[q // g], lambda i: buf.at[i], gp, name)
            pending.append((buf.at[pl.ds(0, gp - 1)], sem_of(name)))
            outs[level + 1][...] = x
            arrive(name, gp)
            s = jnp.sum(buf[:, head, :], axis=0)
            if level == 1:
                blocks = [buf[j, count : 2 * count, :] for j in range(gp)]
                blocks += [buf[j, 2 * count :, :] for j in range(gp)]
                if late:
                    build_ft_middle()
                xu = select(jnp.concatenate(blocks, axis=1), m["ft_middle"][...], 0)
        s = s * mask(level, me // g, 1)
        r = saved[level] - outer(s, bas[level][:, RANK:])
        proj = (shared(level) - outer(s, cross_of(level, child_me))) * mask(level, me // g, 0)
        x = outer(r, blk[level][...]) + outer(proj, bas[level][:, :RANK])
    outs[0][...] = x

    for part, sem in pending:
        wait_for(part, send_sem.at[sem])
    for level in range(3):
        g = size[level]
        p = parts_of[level]
        rp = RANK // p
        n = size[level + 1] // g * p
        idx = me % g
        rs_sem = send_sem.at[sem_of(("rs", level))]
        ag_sem = send_sem.at[sem_of(("cross", level))]
        cross_p, buf = m["cross_p", level], m["cross", level]

        def ag_done():
            for _ in range(g // p - 1):
                wait_for(buf.at[pl.ds(0, n)], ag_sem)
            wait_for(buf.at[pl.ds(0, n - 1)], ag_sem)

        if g == p:
            wait_for(cross_p.at[pl.ds(0, (p - 1) * rp)], rs_sem)
            ag_done()
        else:
            pl.when(idx < p)(lambda: wait_for(cross_p.at[pl.ds(0, (p - 1) * rp)], rs_sem))
            pl.when(idx >= p)(lambda: wait_for(cross_p, rs_sem))
            pl.when(idx < p)(ag_done)


def solution(mesh):
    leaves, across = mesh.shape["leaf"], mesh.shape["grid"]

    def shards(*args):
        levels = [args[8 * i : 8 * i + 8] for i in range(3)]
        root = args[24:30]
        (sl, bl, el, qs, pv, cl, rk, tg) = zip(*levels)
        src = list(sl) + [root[0]]
        blk = list(bl) + [root[1]]
        exp = list(el) + [root[2]]
        bas = list(qs) + [root[3]]
        piv = [v.reshape(1, -1) for v in list(pv) + [root[4]]]
        rnk = list(rk) + [root[5]]
        tgt = [t.reshape(1, -1) for t in tg]
        count = src[0].shape[0]
        ups = [t.shape[1] for t in tgt]
        fronts = [r.shape[0] for r in rnk]
        size = [leaves * across // f for f in fronts]
        for v in src:
            assert v.shape[1] == LANES
        vm = lambda *s: pltpu.VMEM(s, F32)
        bits = lambda *s: pltpu.VMEM(s, BF16)
        total = leaves * across
        plane = size[1]
        planes = total // plane
        nch = [size[i + 1] // size[i] for i in range(3)]
        caps = [max(1, -(-ups[i] // size[i + 1])) for i in range(3)]
        parts = [min(size[i], 16) for i in range(3)]
        ft = (size[2] * 2 * LANES, LANES)
        bufs = {
            "f1": vm(plane, 2 * count, LANES),
            "f2": vm(size[2], 3 * count, LANES),
            "f3a": vm(plane, 3 * count, LANES),
            "f3s": vm(planes, 3 * count, LANES),
            "f3b": vm(planes, 3 * count, LANES),
            "b1a": vm(plane, (nch[2] + 1) * count, LANES),
            "b1s": vm(planes, 2 * count, LANES),
            "b1b": vm(planes, 2 * count, LANES),
            "b2": vm(size[2], 3 * count, LANES),
            "b3": vm(size[1], count, LANES),
            "tgt_middle": vm(size[2], 8, LANES),
            "tgt_upper": vm(plane, 8, LANES),
            "tgt_layer": vm(planes, 8, LANES),
            "bot_middle": bits(2 * LANES, size[2] * LANES),
            "bot_upper": bits(planes * LANES, plane * LANES),
            "ft_middle": bits(*ft),
            "ft_upper": bits(plane * LANES, planes * LANES),
        }
        for name in ("f4", "f5"):
            bufs[name, "a"] = vm(plane, count, LANES)
            bufs[name, "b"] = vm(planes, count, LANES)
        for i in range(3):
            wide = LANES if caps[i] <= 4 else 2 * LANES
            bufs["perm", i] = vm(size[i + 1], max(8, caps[i]), wide)
            bufs["couple", i] = vm(size[i + 1], max(8, caps[i]), wide)
            bufs["cross_p", i] = vm(RANK, RANK)
            bufs["rs", i] = vm(size[i], RANK // parts[i], RANK)
            bufs["cross", i] = vm(nch[i] * parts[i], RANK // parts[i], RANK)
            bufs["gt", i] = vm(nch[i] * RANK, LANES * (1 if i == 2 else 2))
            bufs["zp", i] = vm(size[i], count, LANES)
            bufs["piece", i] = vm(nch[i], count, LANES)
        scratch = list(bufs.values())
        scratch += [pltpu.SemaphoreType.DMA((40,)), pltpu.SemaphoreType.DMA((40,))]
        vspec = pl.BlockSpec(memory_space=pltpu.VMEM)
        sspec = pl.BlockSpec(memory_space=pltpu.SMEM)
        return pl.pallas_call(
            functools.partial(kernel, (leaves, across, size, ups, count, caps), list(bufs)),
            out_shape=[jax.ShapeDtypeStruct(v.shape, F32) for v in src],
            in_specs=[vspec] * 20 + [sspec] * 4 + [vspec] * 6,
            out_specs=[vspec] * 4,
            scratch_shapes=scratch,
            compiler_params=pltpu.CompilerParams(
                collective_id=0, has_side_effects=True, vmem_limit_bytes=60 * 1024 * 1024
            ),
        )(*src, *blk, *exp, *bas, *piv, *rnk, *cl, *tgt)

    spread = ("leaf", "grid")
    level = (P(None, spread), P(spread, None), P(spread, None), P(spread, None), P(spread))
    mid = level + (P(spread, None), P(), P(spread))
    return jax.shard_map(
        shards,
        mesh=mesh,
        in_specs=mid * 3 + level + (P(),),
        out_specs=(P(None, spread),) * 4,
        check_vma=False,
    )
```

```python
import functools

import jax
import jax.numpy as jnp
from jax import lax
from jax.experimental import pallas as pl
from jax.experimental.pallas import tpu as pltpu
from jax.sharding import PartitionSpec as P

RANK = 128
LANES = 128
MESH = pl.DeviceIdType.MESH
F32 = jnp.float32
BF16 = jnp.bfloat16


def once(a, b, ca, cb):
    return lax.dot_general(a, b, (((ca,), (cb,)), ((), ())), preferred_element_type=F32)


def halves(x):
    hi = x.astype(BF16)
    return hi, (x - hi.astype(F32)).astype(BF16)


def dot(a, b, ca, cb):
    ah, al = halves(a)
    bh, bl = halves(b)
    if ca == 0:
        return once(ah, bh, ca, cb) + (once(al, bh, ca, cb) + once(ah, bl, ca, cb))
    n = a.shape[0]
    both = once(jnp.concatenate([ah.astype(F32), al.astype(F32)], axis=0).astype(BF16), bh, ca, cb)
    return both[:n] + (both[n:] + once(ah, bl, ca, cb))


def pieces3(x):
    hi = x.astype(BF16)
    rest = x - hi.astype(F32)
    mid = rest.astype(BF16)
    return hi, mid, (rest - mid.astype(F32)).astype(BF16)


def mult(a, b):
    return dot(a, b, 1, 0)


def outer(a, b):
    return dot(a, b, 1, 1)


def inner(a, b):
    return dot(a, b, 0, 0)


def split3(x):
    hi = x.astype(BF16).astype(F32)
    rest = x - hi
    mid = rest.astype(BF16).astype(F32)
    return jnp.concatenate([hi, mid, rest - mid], axis=0).astype(BF16)


def select(x, onehot, cb):
    out = once(split3(x), onehot, 1, cb)
    n = x.shape[0]
    return out[:n] + out[n : 2 * n] + out[2 * n :]


def kernel(cfg, names, *refs):
    leaves, across, size, ups, count, caps = cfg
    total_devices = leaves * across
    (src, blk, exp, bas, piv, rnk) = [refs[4 * i : 4 * i + 4] for i in range(6)]
    cpl = refs[24:27]
    tgt = refs[27:30]
    outs = refs[30:34]
    m = dict(zip(names, refs[34:-2]))
    send_sem, recv_sem = refs[-2:]
    sems = {}

    me = lax.axis_index("leaf") * across + lax.axis_index("grid")
    plane = size[1]
    planes = total_devices // plane
    spot = me % plane
    layer = me // plane
    late = total_devices > 64
    pending = []

    def where(peer):
        return (peer // across, peer % across)

    def sem_of(name):
        return sems.setdefault(name, len(sems))

    def remote(a, b, sem, peer):
        return pltpu.make_async_remote_copy(
            src_ref=a,
            dst_ref=b,
            send_sem=send_sem.at[sem],
            recv_sem=recv_sem.at[sem],
            device_id=where(peer),
            device_id_type=MESH,
        )

    def wait_for(part, sem):
        pltpu.make_async_copy(part, part, sem).wait()

    def send_each(source, dest, group, name, stride=1):
        idx = me // stride % group
        base = me - idx * stride
        sem = sem_of(name)

        def body(k, carry):
            q = (idx + k) % group
            remote(source(q), dest(idx), sem, base + q * stride).start()
            return carry

        lax.fori_loop(1, group, body, 0)

    def send_all(name, group, stride=1):
        buf = m[name]
        idx = me // stride % group
        send_each(lambda q: buf.at[idx], lambda i: buf.at[i], group, name, stride)
        pending.append((buf.at[pl.ds(0, group - 1)], sem_of(name)))

    def arrive(name, group):
        wait_for(m[name].at[pl.ds(0, group - 1)], recv_sem.at[sem_of(name)])

    barrier = pltpu.get_barrier_semaphore()

    def greet(k, carry):
        pl.semaphore_signal(
            barrier, inc=1, device_id=where((me + k) % total_devices), device_id_type=MESH
        )
        return carry

    lax.fori_loop(1, total_devices, greet, 0)

    col = lax.broadcasted_iota(jnp.int32, (count, RANK), 1)

    def mask(level, front, which):
        return (col < rnk[level][front, which]).astype(F32)

    def local_forward(level, b):
        local = mult(b, blk[level][...])
        bq = mult(b, bas[level][:, :RANK])
        lv = mult(local, bas[level][:, RANK:]) if level < 3 else None
        return local, bq, lv

    parts_of = [min(size[level], 16) for level in range(3)]

    def scatter_cross(level):
        g = size[level]
        p = parts_of[level]
        rp = RANK // p
        idx = me % g
        base = me - idx
        sem = sem_of(("rs", level))
        cross_p, rs_buf = m["cross_p", level], m["rs", level]

        def body(k, carry):
            q = (idx + k) % p

            def go():
                rows = pl.ds(pl.multiple_of(q * rp, 8), rp)
                remote(cross_p.at[rows], rs_buf.at[idx], sem, base + q).start()

            if g == p:
                go()
            else:
                pl.when(q != idx)(go)
            return carry

        lax.fori_loop(1 if g == p else 0, p, body, 0)

        def keep():
            rows = pl.ds(pl.multiple_of(idx * rp, 8), rp)
            rs_buf[idx] = cross_p[rows, :]

        if g == p:
            keep()
        else:
            pl.when(idx < p)(keep)

    def ship_couple(level):
        gp = size[level + 1]
        u = ups[level]
        cap = caps[level]
        wide = max(8, cap)
        sep = gp * LANES
        t = tgt[level][...]
        upd = t >= sep
        rel = jnp.where(upd, t - sep, t)
        dst = rel // LANES
        low = rel % LANES + jnp.where(upd, LANES, 0)
        ri = lax.broadcasted_iota(jnp.int32, (u, u), 0)
        ci = lax.broadcasted_iota(jnp.int32, (u, u), 1)
        dst_f = dst.astype(F32)
        dst_c = jnp.sum(jnp.where(ri == ci, jnp.broadcast_to(dst_f, (u, u)), 0.0), axis=1, keepdims=True)
        rank = jnp.sum(
            jnp.where((dst_c == dst_f) & (ri < ci), 1.0, 0.0), axis=0, keepdims=True
        ).astype(jnp.int32)
        pos = dst * wide + rank
        slots = gp * wide
        si = lax.broadcasted_iota(jnp.int32, (slots, u), 0)
        hit = (si == pos).astype(F32)
        hit16 = hit.astype(BF16)
        hi, mid, lo = [once(hit16, piece, 1, 0) for piece in pieces3(cpl[level][...])]
        moved = hi + mid + lo
        perm_buf, recv_c = m["perm", level], m["couple", level]
        if cap <= 4:
            shifted = (si == pos + 4).astype(F32)
            lowc = jnp.sum(shifted * low.astype(F32), axis=1, keepdims=True)
            both = moved + jnp.broadcast_to(lowc, (slots, LANES))
        else:
            lowc = jnp.sum(hit * low.astype(F32), axis=1, keepdims=True)
            both = jnp.concatenate([moved, jnp.broadcast_to(lowc, (slots, LANES))], axis=1)
        perm_buf[...] = both.reshape(gp, wide, both.shape[1])
        idx = me % gp
        recv_c[idx] = perm_buf[idx]
        send_each(lambda q: perm_buf.at[q], lambda i: recv_c.at[i], gp, ("couple", level))
        pending.append((perm_buf.at[pl.ds(0, gp - 1)], sem_of(("couple", level))))

    def gather_cross(level):
        g = size[level]
        gp = size[level + 1]
        p = parts_of[level]
        idx = me % g
        place = me % gp
        sem = sem_of(("cross", level))
        slot = place // g * p + idx
        buf, rs_buf = m["cross", level], m["rs", level]

        def go():
            wait_for(rs_buf.at[pl.ds(0, g - 1)], recv_sem.at[sem_of(("rs", level))])
            buf[slot] = jnp.sum(rs_buf[...], axis=0)

            def body(k, carry):
                peer = me - place + (place + k) % gp
                remote(buf.at[slot], buf.at[slot], sem, peer).start()
                return carry

            lax.fori_loop(1, gp, body, 0)

        if g == p:
            go()
        else:
            pl.when(idx < p)(go)

    def build_gt(level):
        g = size[level]
        gp = size[level + 1]
        wide = max(8, caps[level])
        nch = gp // g
        gt = m["gt", level]
        rows = gt.shape[1]
        arrive(("couple", level), gp)
        slots = g * wide
        lane = lax.broadcasted_iota(jnp.int32, (slots, rows), 1).astype(F32)
        for child in range(nch):
            got = m["couple", level][child * g : (child + 1) * g]
            got = got.reshape(slots, got.shape[2])
            if caps[level] <= 4:
                up = jnp.concatenate([got[4:, :1], got[:4, :1]], axis=0)
                si = lax.broadcasted_iota(jnp.int32, (slots, 1), 0)
                low = jnp.where(si % 8 < 4, up, -1.0)
            else:
                low = got[:, LANES : LANES + 1]
            ot = (lane == low).astype(F32).astype(BF16)
            hi, mid, lo = [once(piece, ot, 0, 0) for piece in pieces3(got[:, :LANES])]
            gt[child * RANK : (child + 1) * RANK, :] = hi + mid + lo

    def arrive_cross(level):
        g = size[level]
        p = parts_of[level]
        n = size[level + 1] // g * p
        sem = recv_sem.at[sem_of(("cross", level))]
        buf = m["cross", level]
        if g == p:
            wait_for(buf.at[pl.ds(0, n - 1)], sem)
        else:
            idx = me % g
            pl.when(idx < p)(lambda: wait_for(buf.at[pl.ds(0, n - 1)], sem))
            pl.when(idx >= p)(lambda: wait_for(buf.at[pl.ds(0, n)], sem))

    def cross_of(level, child):
        p = parts_of[level]
        return m["cross", level][pl.ds(child * p, p)].reshape(RANK, RANK)

    def build_bot_middle():
        gp = size[2]
        place = me % gp
        rows = 2 * LANES
        ri = lax.broadcasted_iota(jnp.int32, (rows, LANES), 0)
        arrive("tgt_middle", gp)
        mine = jnp.where(ri < LANES, place * LANES + ri, (gp + place - 1) * LANES + ri).astype(F32)

        def fill(j, carry):
            t = m["tgt_middle"][j][0:1, :]
            lanes = pl.ds(pl.multiple_of(j * LANES, LANES), LANES)
            m["bot_middle"][:, lanes] = (mine == t).astype(F32).astype(BF16)
            return carry

        lax.fori_loop(0, gp, fill, 0)

    def build_bot_upper():
        rows = planes * LANES
        ri = lax.broadcasted_iota(jnp.int32, (rows, LANES), 0)
        arrive("tgt_upper", plane)
        mine = ((ri // LANES * plane + spot) * LANES + ri % LANES).astype(F32)

        def fill(j, carry):
            t = m["tgt_upper"][j][0:1, :]
            lanes = pl.ds(pl.multiple_of(j * LANES, LANES), LANES)
            m["bot_upper"][:, lanes] = (mine == t).astype(F32).astype(BF16)
            return carry

        lax.fori_loop(0, plane, fill, 0)

    def build_ft_middle():
        t = tgt[1][...]
        ri = lax.broadcasted_iota(jnp.int32, (LANES, LANES), 0)

        def fill(j, carry):
            rows = pl.ds(pl.multiple_of(j * LANES, LANES), LANES)
            m["ft_middle"][rows, :] = (ri + j * LANES == t).astype(F32).astype(BF16)
            return carry

        lax.fori_loop(0, m["ft_middle"].shape[0] // LANES, fill, 0)

    def build_ft_upper():
        arrive("tgt_layer", planes)
        t = jnp.concatenate([m["tgt_layer"][j][0:1, :] for j in range(planes)], axis=1)
        ri = lax.broadcasted_iota(jnp.int32, (LANES, planes * LANES), 0)

        def fill(j, carry):
            rows = pl.ds(pl.multiple_of(j * LANES, LANES), LANES)
            here = ((ri + (layer * plane + j) * LANES).astype(F32) == t).astype(F32)
            m["ft_upper"][rows, :] = here.astype(BF16)
            return carry

        lax.fori_loop(0, plane, fill, 0)

    def total_sum(value, name):
        m[name, "a"][spot] = value
        send_all((name, "a"), plane)
        arrive((name, "a"), plane)
        m[name, "b"][layer] = jnp.sum(m[name, "a"][...], axis=0)
        send_all((name, "b"), planes, plane)

    def total_arrived(name):
        arrive((name, "b"), planes)
        return jnp.sum(m[name, "b"][...], axis=0)

    def share(level, zp):
        m["zp", level][me % size[level]] = zp
        send_all(("zp", level), size[level])

    def shared(level):
        arrive(("zp", level), size[level])
        return jnp.sum(m["zp", level][...], axis=0)

    local, bq, lv = local_forward(0, src[0][...])
    m["f1"][spot] = jnp.concatenate([bq, lv], axis=0)
    m["cross_p", 0][...] = inner(exp[0][...], bas[0][:, RANK:])
    pl.semaphore_wait(barrier, total_devices - 1)
    send_all("f1", plane)
    scatter_cross(0)
    ship_couple(0)
    for level in (1, 2):
        m["cross_p", level][...] = inner(exp[level][...], bas[level][:, RANK:])
        scatter_cross(level)
    m["tgt_middle"][me % size[2]] = jnp.broadcast_to(tgt[1][...], (8, LANES)).astype(F32)
    send_all("tgt_middle", size[2])
    gather_cross(0)
    ship_couple(1)
    gather_cross(1)
    mine_t = jnp.broadcast_to(tgt[2][...], (8, LANES)).astype(F32)
    m["tgt_upper"][spot] = mine_t
    send_all("tgt_upper", plane)
    m["tgt_layer"][layer] = mine_t
    send_all("tgt_layer", planes, plane)
    build_gt(0)

    saved = []
    inc_upd = None
    for level in range(3):
        g = size[level]
        gp = size[level + 1]
        nch = gp // g
        place = me % gp
        parent = me // gp
        child_me = place // g
        arrive_cross(level)
        if level < 2:
            name = ("f1", "f2")[level]
            buf, step = m[name], g
            arrive(name, gp)
        else:
            buf, step = m["f3b"], g // plane
            arrive("f3b", planes)
        ws = []
        for child in range(nch):
            tot = jnp.sum(buf[child * step : (child + 1) * step, : 2 * count, :], axis=0)
            front = parent * nch + child
            hq = tot[:count] * mask(level, front, 0)
            cross = cross_of(level, child)
            ws.append((tot[count:] + mult(hq, cross)) * mask(level, front, 1))
        inc = -mult(jnp.concatenate(ws, axis=1), m["gt", level][...])
        if level == 1:
            rows = jnp.concatenate([buf[j, 2 * count : 3 * count, :] for j in range(gp)], axis=1)
            inc = inc + select(rows, m["bot_middle"][...], 1)
        if level == 2:
            inc = inc + jnp.sum(buf[:, 2 * count : 3 * count, :], axis=0)
        bn = src[level + 1][...] + inc[:, :LANES]
        local_n, bq_n, lv_n = local_forward(level + 1, bn)
        if level == 0:
            m["f2"][me % size[2]] = jnp.concatenate([bq_n, lv_n, inc[:, LANES:]], axis=0)
            send_all("f2", size[2])
        elif level == 1:
            m["f3a"][spot] = jnp.concatenate([bq_n, lv_n, inc[:, LANES:]], axis=0)
            send_all("f3a", plane)
        else:
            m["f4", "a"][spot] = bq_n
            send_all(("f4", "a"), plane)
        own = jnp.sum(buf[pl.ds(child_me * step, step), :count, :], axis=0)
        hq = own * mask(level, me // g, 0)
        z = (local + outer(hq, exp[level][...])) * piv[level][...]
        saved.append(z)
        share(level, mult(z, exp[level][...]))
        if level == 0:
            ship_couple(2)
            gather_cross(2)
            build_gt(1)
            build_bot_middle()
        elif level == 1:
            build_bot_upper()
            arrive("f3a", plane)
            sums = jnp.sum(m["f3a"][:, : 2 * count, :], axis=0)
            rows = jnp.concatenate([m["f3a"][j, 2 * count :, :] for j in range(plane)], axis=1)
            part = select(rows, m["bot_upper"][...], 1)
            for q in range(planes):
                m["f3s"][q] = jnp.concatenate([sums, part[:, q * LANES : (q + 1) * LANES]], axis=0)
            m["f3b"][layer] = m["f3s"][layer]
            send_each(lambda q: m["f3s"].at[q], lambda i: m["f3b"].at[i], planes, "f3b", plane)
            pending.append((m["f3s"].at[pl.ds(0, planes - 1)], sem_of("f3b")))
            build_gt(2)
        else:
            arrive(("f4", "a"), plane)
            m["f4", "b"][layer] = jnp.sum(m["f4", "a"][...], axis=0)
            send_all(("f4", "b"), planes, plane)
        local = local_n

    build_ft_upper()
    hq = total_arrived("f4") * mask(3, 0, 0)
    z = (local + outer(hq, exp[3][...])) * piv[3][...]
    total_sum(mult(z, exp[3][...]), "f5")
    if not late:
        build_ft_middle()
    x = outer(z, blk[3][...])
    rp_total = total_arrived("f5") * mask(3, 0, 0)
    x = x + outer(rp_total, bas[3][:, :RANK])

    xu = None
    for level in (2, 1, 0):
        g = size[level]
        gp = size[level + 1]
        nch = gp // g
        place = me % gp
        child_me = place // g
        full = x if xu is None else jnp.concatenate([x, xu], axis=1)
        sp = outer(full, m["gt", level][...])
        pieces = [sp[:, c * RANK : (c + 1) * RANK] for c in range(nch)]
        if level == 2:
            m["b1a"][spot] = jnp.concatenate(pieces + [x], axis=0)
            send_all("b1a", plane)
            outs[3][...] = x
            arrive("b1a", plane)
            o = nch * count
            sums = jnp.sum(m["b1a"][:, :o, :], axis=0)
            rows = jnp.concatenate([m["b1a"][j, o:, :] for j in range(plane)], axis=1)
            part = select(rows, m["ft_upper"][...], 0)
            for q in range(planes):
                c = q * plane // g
                m["b1s"][q] = jnp.concatenate(
                    [sums[c * count : (c + 1) * count], part[:, q * LANES : (q + 1) * LANES]], axis=0
                )
            m["b1b"][layer] = m["b1s"][layer]
            send_each(lambda q: m["b1s"].at[q], lambda i: m["b1b"].at[i], planes, "b1b", plane)
            pending.append((m["b1s"].at[pl.ds(0, planes - 1)], sem_of("b1b")))
            arrive("b1b", planes)
            both = jnp.sum(m["b1b"][...], axis=0)
            s, xu = both[:count], both[count:]
        else:
            name = ("b3", "b2")[level]
            buf, piece = m[name], m["piece", level]
            for c in range(nch):
                piece[c] = pieces[c]
            head = pl.ds(0, count)
            rest = pl.ds(count, 2 * count)
            buf[place, head] = piece[child_me]
            if level == 1:
                buf[place, rest] = jnp.concatenate([x, xu], axis=0)

                def ship(k, carry, gp=gp, g=g, place=place, buf=buf, piece=piece, name=name):
                    q = (place + k) % gp
                    peer = me - place + q
                    sem = sem_of(name)
                    remote(piece.at[q // g], buf.at[place, head], sem, peer).start()
                    remote(buf.at[place, rest], buf.at[place, rest], sem, peer).start()
                    return carry

                lax.fori_loop(1, gp, ship, 0)
            else:
                send_each(lambda q: piece.at[q // g], lambda i: buf.at[i], gp, name)
            pending.append((buf.at[pl.ds(0, gp - 1)], sem_of(name)))
            outs[level + 1][...] = x
            arrive(name, gp)
            s = jnp.sum(buf[:, head, :], axis=0)
            if level == 1:
                blocks = [buf[j, count : 2 * count, :] for j in range(gp)]
                blocks += [buf[j, 2 * count :, :] for j in range(gp)]
                if late:
                    build_ft_middle()
                xu = select(jnp.concatenate(blocks, axis=1), m["ft_middle"][...], 0)
        s = s * mask(level, me // g, 1)
        r = saved[level] - outer(s, bas[level][:, RANK:])
        proj = (shared(level) - outer(s, cross_of(level, child_me))) * mask(level, me // g, 0)
        x = outer(r, blk[level][...]) + outer(proj, bas[level][:, :RANK])
    outs[0][...] = x

    for part, sem in pending:
        wait_for(part, send_sem.at[sem])
    for level in range(3):
        g = size[level]
        p = parts_of[level]
        rp = RANK // p
        n = size[level + 1] // g * p
        idx = me % g
        rs_sem = send_sem.at[sem_of(("rs", level))]
        ag_sem = send_sem.at[sem_of(("cross", level))]
        cross_p, buf = m["cross_p", level], m["cross", level]

        def ag_done():
            for _ in range(g // p - 1):
                wait_for(buf.at[pl.ds(0, n)], ag_sem)
            wait_for(buf.at[pl.ds(0, n - 1)], ag_sem)

        if g == p:
            wait_for(cross_p.at[pl.ds(0, (p - 1) * rp)], rs_sem)
            ag_done()
        else:
            pl.when(idx < p)(lambda: wait_for(cross_p.at[pl.ds(0, (p - 1) * rp)], rs_sem))
            pl.when(idx >= p)(lambda: wait_for(cross_p, rs_sem))
            pl.when(idx < p)(ag_done)


def solution(mesh):
    leaves, across = mesh.shape["leaf"], mesh.shape["grid"]

    def shards(*args):
        levels = [args[8 * i : 8 * i + 8] for i in range(3)]
        root = args[24:30]
        (sl, bl, el, qs, pv, cl, rk, tg) = zip(*levels)
        src = list(sl) + [root[0]]
        blk = list(bl) + [root[1]]
        exp = list(el) + [root[2]]
        bas = list(qs) + [root[3]]
        piv = [v.reshape(1, -1) for v in list(pv) + [root[4]]]
        rnk = list(rk) + [root[5]]
        tgt = [t.reshape(1, -1) for t in tg]
        count = src[0].shape[0]
        ups = [t.shape[1] for t in tgt]
        fronts = [r.shape[0] for r in rnk]
        size = [leaves * across // f for f in fronts]
        for v in src:
            assert v.shape[1] == LANES
        vm = lambda *s: pltpu.VMEM(s, F32)
        bits = lambda *s: pltpu.VMEM(s, BF16)
        total = leaves * across
        plane = size[1]
        planes = total // plane
        nch = [size[i + 1] // size[i] for i in range(3)]
        caps = [max(1, -(-ups[i] // size[i + 1])) for i in range(3)]
        parts = [min(size[i], 16) for i in range(3)]
        ft = (size[2] * 2 * LANES, LANES)
        bufs = {
            "f1": vm(plane, 2 * count, LANES),
            "f2": vm(size[2], 3 * count, LANES),
            "f3a": vm(plane, 3 * count, LANES),
            "f3s": vm(planes, 3 * count, LANES),
            "f3b": vm(planes, 3 * count, LANES),
            "b1a": vm(plane, (nch[2] + 1) * count, LANES),
            "b1s": vm(planes, 2 * count, LANES),
            "b1b": vm(planes, 2 * count, LANES),
            "b2": vm(size[2], 3 * count, LANES),
            "b3": vm(size[1], count, LANES),
            "tgt_middle": vm(size[2], 8, LANES),
            "tgt_upper": vm(plane, 8, LANES),
            "tgt_layer": vm(planes, 8, LANES),
            "bot_middle": bits(2 * LANES, size[2] * LANES),
            "bot_upper": bits(planes * LANES, plane * LANES),
            "ft_middle": bits(*ft),
            "ft_upper": bits(plane * LANES, planes * LANES),
        }
        for name in ("f4", "f5"):
            bufs[name, "a"] = vm(plane, count, LANES)
            bufs[name, "b"] = vm(planes, count, LANES)
        for i in range(3):
            wide = LANES if caps[i] <= 4 else 2 * LANES
            bufs["perm", i] = vm(size[i + 1], max(8, caps[i]), wide)
            bufs["couple", i] = vm(size[i + 1], max(8, caps[i]), wide)
            bufs["cross_p", i] = vm(RANK, RANK)
            bufs["rs", i] = vm(size[i], RANK // parts[i], RANK)
            bufs["cross", i] = vm(nch[i] * parts[i], RANK // parts[i], RANK)
            bufs["gt", i] = vm(nch[i] * RANK, LANES * (1 if i == 2 else 2))
            bufs["zp", i] = vm(size[i], count, LANES)
            bufs["piece", i] = vm(nch[i], count, LANES)
        scratch = list(bufs.values())
        scratch += [pltpu.SemaphoreType.DMA((40,)), pltpu.SemaphoreType.DMA((40,))]
        vspec = pl.BlockSpec(memory_space=pltpu.VMEM)
        sspec = pl.BlockSpec(memory_space=pltpu.SMEM)
        return pl.pallas_call(
            functools.partial(kernel, (leaves, across, size, ups, count, caps), list(bufs)),
            out_shape=[jax.ShapeDtypeStruct(v.shape, F32) for v in src],
            in_specs=[vspec] * 20 + [sspec] * 4 + [vspec] * 6,
            out_specs=[vspec] * 4,
            scratch_shapes=scratch,
            compiler_params=pltpu.CompilerParams(
                collective_id=0, has_side_effects=True, vmem_limit_bytes=60 * 1024 * 1024
            ),
        )(*src, *blk, *exp, *bas, *piv, *rnk, *cl, *tgt)

    spread = ("leaf", "grid")
    level = (P(None, spread), P(spread, None), P(spread, None), P(spread, None), P(spread))
    mid = level + (P(spread, None), P(), P(spread))
    return jax.shard_map(
        shards,
        mesh=mesh,
        in_specs=mid * 3 + level + (P(),),
        out_specs=(P(None, spread),) * 4,
        check_vma=False,
    )
```

```python
import functools

import jax
import jax.numpy as jnp
from jax import lax
from jax.experimental import pallas as pl
from jax.experimental.pallas import tpu as pltpu
from jax.sharding import PartitionSpec as P

RANK = 128
LANES = 128
MESH = pl.DeviceIdType.MESH
F32 = jnp.float32
BF16 = jnp.bfloat16


def once(a, b, ca, cb):
    return lax.dot_general(a, b, (((ca,), (cb,)), ((), ())), preferred_element_type=F32)


def halves(x):
    hi = x.astype(BF16)
    return hi, (x - hi.astype(F32)).astype(BF16)


def dot(a, b, ca, cb):
    ah, al = halves(a)
    bh, bl = halves(b)
    if ca == 0:
        return once(ah, bh, ca, cb) + (once(al, bh, ca, cb) + once(ah, bl, ca, cb))
    n = a.shape[0]
    both = once(jnp.concatenate([ah.astype(F32), al.astype(F32)], axis=0).astype(BF16), bh, ca, cb)
    return both[:n] + (both[n:] + once(ah, bl, ca, cb))


def pieces3(x):
    hi = x.astype(BF16)
    rest = x - hi.astype(F32)
    mid = rest.astype(BF16)
    return hi, mid, (rest - mid.astype(F32)).astype(BF16)


def mult(a, b):
    return dot(a, b, 1, 0)


def outer(a, b):
    return dot(a, b, 1, 1)


def inner(a, b):
    return dot(a, b, 0, 0)


def split3(x):
    hi = x.astype(BF16).astype(F32)
    rest = x - hi
    mid = rest.astype(BF16).astype(F32)
    return jnp.concatenate([hi, mid, rest - mid], axis=0).astype(BF16)


def select(x, onehot, cb):
    out = once(split3(x), onehot, 1, cb)
    n = x.shape[0]
    return out[:n] + out[n : 2 * n] + out[2 * n :]


def kernel(cfg, names, *refs):
    leaves, across, size, ups, count, caps = cfg
    total_devices = leaves * across
    (src, blk, exp, bas, piv, rnk) = [refs[4 * i : 4 * i + 4] for i in range(6)]
    cpl = refs[24:27]
    tgt = refs[27:30]
    outs = refs[30:34]
    m = dict(zip(names, refs[34:-2]))
    send_sem, recv_sem = refs[-2:]
    sems = {}

    me = lax.axis_index("leaf") * across + lax.axis_index("grid")
    plane = size[1]
    planes = total_devices // plane
    spot = me % plane
    layer = me // plane
    late = total_devices > 64
    pending = []

    def where(peer):
        return (peer // across, peer % across)

    def sem_of(name):
        return sems.setdefault(name, len(sems))

    def remote(a, b, sem, peer):
        return pltpu.make_async_remote_copy(
            src_ref=a,
            dst_ref=b,
            send_sem=send_sem.at[sem],
            recv_sem=recv_sem.at[sem],
            device_id=where(peer),
            device_id_type=MESH,
        )

    def wait_for(part, sem):
        pltpu.make_async_copy(part, part, sem).wait()

    def send_each(source, dest, group, name, stride=1):
        idx = me // stride % group
        base = me - idx * stride
        sem = sem_of(name)

        def body(k, carry):
            q = (idx + k) % group
            remote(source(q), dest(idx), sem, base + q * stride).start()
            return carry

        lax.fori_loop(1, group, body, 0)

    def send_all(name, group, stride=1):
        buf = m[name]
        idx = me // stride % group
        send_each(lambda q: buf.at[idx], lambda i: buf.at[i], group, name, stride)
        pending.append((buf.at[pl.ds(0, group - 1)], sem_of(name)))

    def arrive(name, group):
        wait_for(m[name].at[pl.ds(0, group - 1)], recv_sem.at[sem_of(name)])

    barrier = pltpu.get_barrier_semaphore()

    def greet(k, carry):
        pl.semaphore_signal(
            barrier, inc=1, device_id=where((me + k) % total_devices), device_id_type=MESH
        )
        return carry

    lax.fori_loop(1, total_devices, greet, 0)

    col = lax.broadcasted_iota(jnp.int32, (count, RANK), 1)

    def mask(level, front, which):
        return (col < rnk[level][front, which]).astype(F32)

    def local_forward(level, b):
        local = mult(b, blk[level][...])
        bq = mult(b, bas[level][:, :RANK])
        lv = mult(local, bas[level][:, RANK:]) if level < 3 else None
        return local, bq, lv

    parts_of = [min(size[level], 16) for level in range(3)]

    def scatter_cross(level):
        g = size[level]
        p = parts_of[level]
        rp = RANK // p
        idx = me % g
        base = me - idx
        sem = sem_of(("rs", level))
        cross_p, rs_buf = m["cross_p", level], m["rs", level]

        def body(k, carry):
            q = (idx + k) % p

            def go():
                rows = pl.ds(pl.multiple_of(q * rp, 8), rp)
                remote(cross_p.at[rows], rs_buf.at[idx], sem, base + q).start()

            if g == p:
                go()
            else:
                pl.when(q != idx)(go)
            return carry

        lax.fori_loop(1 if g == p else 0, p, body, 0)

        def keep():
            rows = pl.ds(pl.multiple_of(idx * rp, 8), rp)
            rs_buf[idx] = cross_p[rows, :]

        if g == p:
            keep()
        else:
            pl.when(idx < p)(keep)

    def pack_couple(level):
        gp = size[level + 1]
        u = ups[level]
        cap = caps[level]
        wide = max(8, cap)
        sep = gp * LANES
        t = tgt[level][...]
        upd = t >= sep
        rel = jnp.where(upd, t - sep, t)
        dst = rel // LANES
        low = rel % LANES + jnp.where(upd, LANES, 0)
        ri = lax.broadcasted_iota(jnp.int32, (u, u), 0)
        ci = lax.broadcasted_iota(jnp.int32, (u, u), 1)
        dst_f = dst.astype(F32)
        dst_c = jnp.sum(jnp.where(ri == ci, jnp.broadcast_to(dst_f, (u, u)), 0.0), axis=1, keepdims=True)
        rank = jnp.sum(
            jnp.where((dst_c == dst_f) & (ri < ci), 1.0, 0.0), axis=0, keepdims=True
        ).astype(jnp.int32)
        pos = dst * wide + rank
        slots = gp * wide
        si = lax.broadcasted_iota(jnp.int32, (slots, u), 0)
        hit = (si == pos).astype(F32)
        hit16 = hit.astype(BF16)
        hi, mid, lo = [once(hit16, piece, 1, 0) for piece in pieces3(cpl[level][...])]
        moved = hi + mid + lo
        perm_buf, recv_c = m["perm", level], m["couple", level]
        if cap <= 4:
            shifted = (si == pos + 4).astype(F32)
            lowc = jnp.sum(shifted * low.astype(F32), axis=1, keepdims=True)
            both = moved + jnp.broadcast_to(lowc, (slots, LANES))
        else:
            lowc = jnp.sum(hit * low.astype(F32), axis=1, keepdims=True)
            both = jnp.concatenate([moved, jnp.broadcast_to(lowc, (slots, LANES))], axis=1)
        perm_buf[...] = both.reshape(gp, wide, both.shape[1])
        idx = me % gp
        recv_c[idx] = perm_buf[idx]

    def ship_couple(level):
        gp = size[level + 1]
        perm_buf, recv_c = m["perm", level], m["couple", level]
        send_each(lambda q: perm_buf.at[q], lambda i: recv_c.at[i], gp, ("couple", level))
        pending.append((perm_buf.at[pl.ds(0, gp - 1)], sem_of(("couple", level))))

    def gather_cross(level):
        g = size[level]
        gp = size[level + 1]
        p = parts_of[level]
        idx = me % g
        place = me % gp
        sem = sem_of(("cross", level))
        slot = place // g * p + idx
        buf, rs_buf = m["cross", level], m["rs", level]

        def go():
            wait_for(rs_buf.at[pl.ds(0, g - 1)], recv_sem.at[sem_of(("rs", level))])
            buf[slot] = jnp.sum(rs_buf[...], axis=0)

            def body(k, carry):
                peer = me - place + (place + k) % gp
                remote(buf.at[slot], buf.at[slot], sem, peer).start()
                return carry

            lax.fori_loop(1, gp, body, 0)

        if g == p:
            go()
        else:
            pl.when(idx < p)(go)

    def build_gt(level):
        g = size[level]
        gp = size[level + 1]
        wide = max(8, caps[level])
        nch = gp // g
        gt = m["gt", level]
        rows = gt.shape[1]
        arrive(("couple", level), gp)
        slots = g * wide
        lane = lax.broadcasted_iota(jnp.int32, (slots, rows), 1).astype(F32)
        for child in range(nch):
            got = m["couple", level][child * g : (child + 1) * g]
            got = got.reshape(slots, got.shape[2])
            if caps[level] <= 4:
                up = jnp.concatenate([got[4:, :1], got[:4, :1]], axis=0)
                si = lax.broadcasted_iota(jnp.int32, (slots, 1), 0)
                low = jnp.where(si % 8 < 4, up, -1.0)
            else:
                low = got[:, LANES : LANES + 1]
            ot = (lane == low).astype(F32).astype(BF16)
            hi, mid, lo = [once(piece, ot, 0, 0) for piece in pieces3(got[:, :LANES])]
            gt[child * RANK : (child + 1) * RANK, :] = hi + mid + lo

    def arrive_cross(level):
        g = size[level]
        p = parts_of[level]
        n = size[level + 1] // g * p
        sem = recv_sem.at[sem_of(("cross", level))]
        buf = m["cross", level]
        if g == p:
            wait_for(buf.at[pl.ds(0, n - 1)], sem)
        else:
            idx = me % g
            pl.when(idx < p)(lambda: wait_for(buf.at[pl.ds(0, n - 1)], sem))
            pl.when(idx >= p)(lambda: wait_for(buf.at[pl.ds(0, n)], sem))

    def cross_of(level, child):
        p = parts_of[level]
        return m["cross", level][pl.ds(child * p, p)].reshape(RANK, RANK)

    def build_bot_middle():
        gp = size[2]
        place = me % gp
        rows = 2 * LANES
        ri = lax.broadcasted_iota(jnp.int32, (rows, LANES), 0)
        arrive("tgt_middle", gp)
        mine = jnp.where(ri < LANES, place * LANES + ri, (gp + place - 1) * LANES + ri).astype(F32)

        def fill(j, carry):
            t = m["tgt_middle"][j][0:1, :]
            lanes = pl.ds(pl.multiple_of(j * LANES, LANES), LANES)
            m["bot_middle"][:, lanes] = (mine == t).astype(F32).astype(BF16)
            return carry

        lax.fori_loop(0, gp, fill, 0)

    def build_bot_upper():
        rows = planes * LANES
        ri = lax.broadcasted_iota(jnp.int32, (rows, LANES), 0)
        arrive("tgt_upper", plane)
        mine = ((ri // LANES * plane + spot) * LANES + ri % LANES).astype(F32)

        def fill(j, carry):
            t = m["tgt_upper"][j][0:1, :]
            lanes = pl.ds(pl.multiple_of(j * LANES, LANES), LANES)
            m["bot_upper"][:, lanes] = (mine == t).astype(F32).astype(BF16)
            return carry

        lax.fori_loop(0, plane, fill, 0)

    def build_ft_middle():
        t = tgt[1][...]
        ri = lax.broadcasted_iota(jnp.int32, (LANES, LANES), 0)

        def fill(j, carry):
            rows = pl.ds(pl.multiple_of(j * LANES, LANES), LANES)
            m["ft_middle"][rows, :] = (ri + j * LANES == t).astype(F32).astype(BF16)
            return carry

        lax.fori_loop(0, m["ft_middle"].shape[0] // LANES, fill, 0)

    def build_ft_upper():
        arrive("tgt_layer", planes)
        t = jnp.concatenate([m["tgt_layer"][j][0:1, :] for j in range(planes)], axis=1)
        ri = lax.broadcasted_iota(jnp.int32, (LANES, planes * LANES), 0)

        def fill(j, carry):
            rows = pl.ds(pl.multiple_of(j * LANES, LANES), LANES)
            here = ((ri + (layer * plane + j) * LANES).astype(F32) == t).astype(F32)
            m["ft_upper"][rows, :] = here.astype(BF16)
            return carry

        lax.fori_loop(0, plane, fill, 0)

    def total_sum(value, name):
        m[name, "a"][spot] = value
        send_all((name, "a"), plane)
        arrive((name, "a"), plane)
        m[name, "b"][layer] = jnp.sum(m[name, "a"][...], axis=0)
        send_all((name, "b"), planes, plane)

    def total_arrived(name):
        arrive((name, "b"), planes)
        return jnp.sum(m[name, "b"][...], axis=0)

    def share(level, zp):
        m["zp", level][me % size[level]] = zp
        send_all(("zp", level), size[level])

    def shared(level):
        arrive(("zp", level), size[level])
        return jnp.sum(m["zp", level][...], axis=0)

    local, bq, lv = local_forward(0, src[0][...])
    m["f1"][spot] = jnp.concatenate([bq, lv], axis=0)
    for level in range(3):
        m["cross_p", level][...] = inner(exp[level][...], bas[level][:, RANK:])
        pack_couple(level)
    pl.semaphore_wait(barrier, total_devices - 1)
    send_all("f1", plane)
    scatter_cross(0)
    ship_couple(0)
    for level in (1, 2):
        scatter_cross(level)
    m["tgt_middle"][me % size[2]] = jnp.broadcast_to(tgt[1][...], (8, LANES)).astype(F32)
    send_all("tgt_middle", size[2])
    gather_cross(0)
    ship_couple(1)
    gather_cross(1)
    mine_t = jnp.broadcast_to(tgt[2][...], (8, LANES)).astype(F32)
    m["tgt_upper"][spot] = mine_t
    send_all("tgt_upper", plane)
    m["tgt_layer"][layer] = mine_t
    send_all("tgt_layer", planes, plane)
    build_gt(0)

    saved = []
    inc_upd = None
    for level in range(3):
        g = size[level]
        gp = size[level + 1]
        nch = gp // g
        place = me % gp
        parent = me // gp
        child_me = place // g
        arrive_cross(level)
        if level < 2:
            name = ("f1", "f2")[level]
            buf, step = m[name], g
            arrive(name, gp)
        else:
            buf, step = m["f3b"], g // plane
            arrive("f3b", planes)
        ws = []
        for child in range(nch):
            tot = jnp.sum(buf[child * step : (child + 1) * step, : 2 * count, :], axis=0)
            front = parent * nch + child
            hq = tot[:count] * mask(level, front, 0)
            cross = cross_of(level, child)
            ws.append((tot[count:] + mult(hq, cross)) * mask(level, front, 1))
        inc = -mult(jnp.concatenate(ws, axis=1), m["gt", level][...])
        if level == 1:
            rows = jnp.concatenate([buf[j, 2 * count : 3 * count, :] for j in range(gp)], axis=1)
            inc = inc + select(rows, m["bot_middle"][...], 1)
        if level == 2:
            inc = inc + jnp.sum(buf[:, 2 * count : 3 * count, :], axis=0)
        bn = src[level + 1][...] + inc[:, :LANES]
        local_n, bq_n, lv_n = local_forward(level + 1, bn)
        if level == 0:
            m["f2"][me % size[2]] = jnp.concatenate([bq_n, lv_n, inc[:, LANES:]], axis=0)
            send_all("f2", size[2])
        elif level == 1:
            m["f3a"][spot] = jnp.concatenate([bq_n, lv_n, inc[:, LANES:]], axis=0)
            send_all("f3a", plane)
        else:
            m["f4", "a"][spot] = bq_n
            send_all(("f4", "a"), plane)
        own = jnp.sum(buf[pl.ds(child_me * step, step), :count, :], axis=0)
        hq = own * mask(level, me // g, 0)
        z = (local + outer(hq, exp[level][...])) * piv[level][...]
        saved.append(z)
        share(level, mult(z, exp[level][...]))
        if level == 0:
            ship_couple(2)
            gather_cross(2)
            build_gt(1)
            build_bot_middle()
        elif level == 1:
            build_bot_upper()
            arrive("f3a", plane)
            sums = jnp.sum(m["f3a"][:, : 2 * count, :], axis=0)
            rows = jnp.concatenate([m["f3a"][j, 2 * count :, :] for j in range(plane)], axis=1)
            part = select(rows, m["bot_upper"][...], 1)
            for q in range(planes):
                m["f3s"][q] = jnp.concatenate([sums, part[:, q * LANES : (q + 1) * LANES]], axis=0)
            m["f3b"][layer] = m["f3s"][layer]
            send_each(lambda q: m["f3s"].at[q], lambda i: m["f3b"].at[i], planes, "f3b", plane)
            pending.append((m["f3s"].at[pl.ds(0, planes - 1)], sem_of("f3b")))
            build_gt(2)
        else:
            arrive(("f4", "a"), plane)
            m["f4", "b"][layer] = jnp.sum(m["f4", "a"][...], axis=0)
            send_all(("f4", "b"), planes, plane)
        local = local_n

    build_ft_upper()
    hq = total_arrived("f4") * mask(3, 0, 0)
    z = (local + outer(hq, exp[3][...])) * piv[3][...]
    total_sum(mult(z, exp[3][...]), "f5")
    if not late:
        build_ft_middle()
    x = outer(z, blk[3][...])
    rp_total = total_arrived("f5") * mask(3, 0, 0)
    x = x + outer(rp_total, bas[3][:, :RANK])

    xu = None
    for level in (2, 1, 0):
        g = size[level]
        gp = size[level + 1]
        nch = gp // g
        place = me % gp
        child_me = place // g
        full = x if xu is None else jnp.concatenate([x, xu], axis=1)
        sp = outer(full, m["gt", level][...])
        pieces = [sp[:, c * RANK : (c + 1) * RANK] for c in range(nch)]
        if level == 2:
            m["b1a"][spot] = jnp.concatenate(pieces + [x], axis=0)
            send_all("b1a", plane)
            outs[3][...] = x
            arrive("b1a", plane)
            o = nch * count
            sums = jnp.sum(m["b1a"][:, :o, :], axis=0)
            rows = jnp.concatenate([m["b1a"][j, o:, :] for j in range(plane)], axis=1)
            part = select(rows, m["ft_upper"][...], 0)
            for q in range(planes):
                c = q * plane // g
                m["b1s"][q] = jnp.concatenate(
                    [sums[c * count : (c + 1) * count], part[:, q * LANES : (q + 1) * LANES]], axis=0
                )
            m["b1b"][layer] = m["b1s"][layer]
            send_each(lambda q: m["b1s"].at[q], lambda i: m["b1b"].at[i], planes, "b1b", plane)
            pending.append((m["b1s"].at[pl.ds(0, planes - 1)], sem_of("b1b")))
            arrive("b1b", planes)
            both = jnp.sum(m["b1b"][...], axis=0)
            s, xu = both[:count], both[count:]
        else:
            name = ("b3", "b2")[level]
            buf, piece = m[name], m["piece", level]
            for c in range(nch):
                piece[c] = pieces[c]
            head = pl.ds(0, count)
            rest = pl.ds(count, 2 * count)
            buf[place, head] = piece[child_me]
            if level == 1:
                buf[place, rest] = jnp.concatenate([x, xu], axis=0)

                def ship(k, carry, gp=gp, g=g, place=place, buf=buf, piece=piece, name=name):
                    q = (place + k) % gp
                    peer = me - place + q
                    sem = sem_of(name)
                    remote(piece.at[q // g], buf.at[place, head], sem, peer).start()
                    remote(buf.at[place, rest], buf.at[place, rest], sem, peer).start()
                    return carry

                lax.fori_loop(1, gp, ship, 0)
            else:
                send_each(lambda q: piece.at[q // g], lambda i: buf.at[i], gp, name)
            pending.append((buf.at[pl.ds(0, gp - 1)], sem_of(name)))
            outs[level + 1][...] = x
            arrive(name, gp)
            s = jnp.sum(buf[:, head, :], axis=0)
            if level == 1:
                blocks = [buf[j, count : 2 * count, :] for j in range(gp)]
                blocks += [buf[j, 2 * count :, :] for j in range(gp)]
                if late:
                    build_ft_middle()
                xu = select(jnp.concatenate(blocks, axis=1), m["ft_middle"][...], 0)
        s = s * mask(level, me // g, 1)
        r = saved[level] - outer(s, bas[level][:, RANK:])
        proj = (shared(level) - outer(s, cross_of(level, child_me))) * mask(level, me // g, 0)
        x = outer(r, blk[level][...]) + outer(proj, bas[level][:, :RANK])
    outs[0][...] = x

    for part, sem in pending:
        wait_for(part, send_sem.at[sem])
    for level in range(3):
        g = size[level]
        p = parts_of[level]
        rp = RANK // p
        n = size[level + 1] // g * p
        idx = me % g
        rs_sem = send_sem.at[sem_of(("rs", level))]
        ag_sem = send_sem.at[sem_of(("cross", level))]
        cross_p, buf = m["cross_p", level], m["cross", level]

        def ag_done():
            for _ in range(g // p - 1):
                wait_for(buf.at[pl.ds(0, n)], ag_sem)
            wait_for(buf.at[pl.ds(0, n - 1)], ag_sem)

        if g == p:
            wait_for(cross_p.at[pl.ds(0, (p - 1) * rp)], rs_sem)
            ag_done()
        else:
            pl.when(idx < p)(lambda: wait_for(cross_p.at[pl.ds(0, (p - 1) * rp)], rs_sem))
            pl.when(idx >= p)(lambda: wait_for(cross_p, rs_sem))
            pl.when(idx < p)(ag_done)


def solution(mesh):
    leaves, across = mesh.shape["leaf"], mesh.shape["grid"]

    def shards(*args):
        levels = [args[8 * i : 8 * i + 8] for i in range(3)]
        root = args[24:30]
        (sl, bl, el, qs, pv, cl, rk, tg) = zip(*levels)
        src = list(sl) + [root[0]]
        blk = list(bl) + [root[1]]
        exp = list(el) + [root[2]]
        bas = list(qs) + [root[3]]
        piv = [v.reshape(1, -1) for v in list(pv) + [root[4]]]
        rnk = list(rk) + [root[5]]
        tgt = [t.reshape(1, -1) for t in tg]
        count = src[0].shape[0]
        ups = [t.shape[1] for t in tgt]
        fronts = [r.shape[0] for r in rnk]
        size = [leaves * across // f for f in fronts]
        for v in src:
            assert v.shape[1] == LANES
        vm = lambda *s: pltpu.VMEM(s, F32)
        bits = lambda *s: pltpu.VMEM(s, BF16)
        total = leaves * across
        plane = size[1]
        planes = total // plane
        nch = [size[i + 1] // size[i] for i in range(3)]
        caps = [max(1, -(-ups[i] // size[i + 1])) for i in range(3)]
        parts = [min(size[i], 16) for i in range(3)]
        ft = (size[2] * 2 * LANES, LANES)
        bufs = {
            "f1": vm(plane, 2 * count, LANES),
            "f2": vm(size[2], 3 * count, LANES),
            "f3a": vm(plane, 3 * count, LANES),
            "f3s": vm(planes, 3 * count, LANES),
            "f3b": vm(planes, 3 * count, LANES),
            "b1a": vm(plane, (nch[2] + 1) * count, LANES),
            "b1s": vm(planes, 2 * count, LANES),
            "b1b": vm(planes, 2 * count, LANES),
            "b2": vm(size[2], 3 * count, LANES),
            "b3": vm(size[1], count, LANES),
            "tgt_middle": vm(size[2], 8, LANES),
            "tgt_upper": vm(plane, 8, LANES),
            "tgt_layer": vm(planes, 8, LANES),
            "bot_middle": bits(2 * LANES, size[2] * LANES),
            "bot_upper": bits(planes * LANES, plane * LANES),
            "ft_middle": bits(*ft),
            "ft_upper": bits(plane * LANES, planes * LANES),
        }
        for name in ("f4", "f5"):
            bufs[name, "a"] = vm(plane, count, LANES)
            bufs[name, "b"] = vm(planes, count, LANES)
        for i in range(3):
            wide = LANES if caps[i] <= 4 else 2 * LANES
            bufs["perm", i] = vm(size[i + 1], max(8, caps[i]), wide)
            bufs["couple", i] = vm(size[i + 1], max(8, caps[i]), wide)
            bufs["cross_p", i] = vm(RANK, RANK)
            bufs["rs", i] = vm(size[i], RANK // parts[i], RANK)
            bufs["cross", i] = vm(nch[i] * parts[i], RANK // parts[i], RANK)
            bufs["gt", i] = vm(nch[i] * RANK, LANES * (1 if i == 2 else 2))
            bufs["zp", i] = vm(size[i], count, LANES)
            bufs["piece", i] = vm(nch[i], count, LANES)
        scratch = list(bufs.values())
        scratch += [pltpu.SemaphoreType.DMA((40,)), pltpu.SemaphoreType.DMA((40,))]
        vspec = pl.BlockSpec(memory_space=pltpu.VMEM)
        sspec = pl.BlockSpec(memory_space=pltpu.SMEM)
        return pl.pallas_call(
            functools.partial(kernel, (leaves, across, size, ups, count, caps), list(bufs)),
            out_shape=[jax.ShapeDtypeStruct(v.shape, F32) for v in src],
            in_specs=[vspec] * 20 + [sspec] * 4 + [vspec] * 6,
            out_specs=[vspec] * 4,
            scratch_shapes=scratch,
            compiler_params=pltpu.CompilerParams(
                collective_id=0, has_side_effects=True, vmem_limit_bytes=60 * 1024 * 1024
            ),
        )(*src, *blk, *exp, *bas, *piv, *rnk, *cl, *tgt)

    spread = ("leaf", "grid")
    level = (P(None, spread), P(spread, None), P(spread, None), P(spread, None), P(spread))
    mid = level + (P(spread, None), P(), P(spread))
    return jax.shard_map(
        shards,
        mesh=mesh,
        in_specs=mid * 3 + level + (P(),),
        out_specs=(P(None, spread),) * 4,
        check_vma=False,
    )
```
